128 devices in a mesh: row: 8 (over z_lo, x), col: 16 (over z_hi, y, core).
Axes of the slice: x: 4, y: 4, z: 4 (z_hi: 2, z_lo: 2; z = z_hi * 2 + z_lo), core: 2. Of those that a mesh axis runs over, the one named last changes fastest.
Arguments:
- x_iterate: float32 [4096, 4096], P('row', 'col'), may hold values from -6 to 6
- z_inverse: float32 [4096, 4096], P('row', 'col'), may hold values from -0.25 to 0.25
- edge_src: int32 [16, 16, 64], P('row', 'col'), may hold values from 0 to 255
- edge_dst: int32 [16, 16, 64], P('row', 'col'), may hold values from 0 to 255
- edge_count: int32 [16, 16], P('row', 'col'), may hold values from 1 to 64, as said below
Outputs:
- schur_row: float32 [16, 16, 64], P('row', 'col')
The draws below stay inside these ranges and needn't reach their ends.
Inputs may be any that keep to these rules, and one draw needn't show every extreme that they name: `edge_count`: slots at and beyond a block pair's count are ignored; some block pair has all 64 slots live in every draw.
All inputs are finite; a program needn't handle non-finite values.
Results may differ from the reference program's by a relative error of at most 0.0001.
Values sent between devices are 32-bit elements; how exact they have to be, the bound alone decides.
A program may use at most 64 MiB of HBM per device.

```python
import jax
import jax.numpy as jnp
from jax import lax

BLOCK = 256
CAP = 64
STEPS = 2
GRID = 16
ORDER = 4096


def draw_edge_count(key, part):
    key_one = jax.random.fold_in(key, 11)
    key_two = jax.random.fold_in(key, 23)
    key_three = jax.random.fold_in(key, 37)
    first = jax.random.randint(key_one, (GRID, GRID), 0, CAP)
    second = jax.random.randint(key_two, (GRID, GRID), 0, CAP)
    counts = CAP - first * second // (2 * CAP)
    chosen = jax.random.randint(key_three, (), 0, GRID * GRID)
    counts = counts.reshape(-1).at[chosen].set(CAP)
    return counts.reshape(GRID, GRID).astype(jnp.int32)


def with_ends(drawn, stream_key, least, largest):
    longest = drawn.shape.index(max(drawn.shape))
    spots = []
    for shift in (0, 1):
        where = [jax.random.randint(jax.random.fold_in(stream_key, axis), (), 0, length) for axis, length in enumerate(drawn.shape)]
        where[longest] = (where[longest] + shift) % drawn.shape[longest]
        spots.append(tuple(where))
    return drawn.at[spots[0]].set(least).at[spots[1]].set(largest)


def level_of(stream_key, shape, pieces, smallest, top_value):
    level = 1.0
    for dim, parts in pieces:
        heights = jax.random.uniform(jax.random.fold_in(jax.random.fold_in(stream_key, 6), dim), (parts,), jnp.float32, smallest / len(pieces), top_value / len(pieces))
        level = level * jnp.repeat(jnp.exp(heights), shape[dim] // parts).reshape((-1,) + (1,) * (len(shape) - 1 - dim))
    return level


def scatter_about(own_key, shape, spread, reach, pieces=(), kind=jnp.bfloat16):
    entries = jax.random.normal(own_key, shape, jnp.float32) * spread
    if len(pieces) > 0:
        entries = level_of(own_key, shape, pieces, -0.22, 0.18) * entries
    return jnp.clip(entries, min=-reach, max=reach).astype(kind)


def setup_inputs(seed: int = 0) -> dict:
    keys = jax.random.split(jax.random.key(seed), 6)
    x_iterate = scatter_about(keys[0], (ORDER, ORDER), 1.0, 6.0, ((0, 8), (1, 16)), jnp.float32)
    z_inverse = scatter_about(keys[1], (ORDER, ORDER), (2 * BLOCK) ** -0.5, 0.25, ((0, 8), (1, 16)), jnp.float32)
    edge_src = with_ends(jax.random.randint(keys[2], (GRID, GRID, CAP), 0, BLOCK), jax.random.fold_in(keys[2], 1), 0, BLOCK - 1).astype(jnp.int32)
    edge_dst = with_ends(jax.random.randint(keys[3], (GRID, GRID, CAP), 0, BLOCK), jax.random.fold_in(keys[3], 1), 0, BLOCK - 1).astype(jnp.int32)
    edge_count = draw_edge_count(jax.random.fold_in(keys[5], 71), 0)
    return {"x_iterate": x_iterate, "z_inverse": z_inverse, "edge_src": edge_src, "edge_dst": edge_dst, "edge_count": edge_count}


def reference(x_iterate, z_inverse, edge_src, edge_dst, edge_count):
    x_blocks = x_iterate.reshape(GRID, BLOCK, GRID, BLOCK).transpose(0, 2, 1, 3)
    z_blocks = z_inverse.reshape(GRID, BLOCK, GRID, BLOCK).transpose(0, 2, 1, 3)
    first = jnp.arange(GRID, dtype=jnp.int32)[:, None]
    second = jnp.arange(GRID, dtype=jnp.int32)[None, :]
    product = jnp.zeros((GRID, GRID, BLOCK, BLOCK), jnp.float32)
    for step in range(STEPS):
        inner = ((first + second + step) % GRID).astype(jnp.int32)
        left = x_blocks[first, inner]
        right = z_blocks[inner, second]
        product = product + jnp.einsum("ijab,ijbc->ijac", left, right, precision=lax.Precision.HIGHEST)
    flat = product.reshape(GRID, GRID, BLOCK * BLOCK)
    index = (edge_src * BLOCK + edge_dst).astype(jnp.int32)
    values = jnp.take_along_axis(flat, index, axis=2)
    live = jnp.arange(CAP, dtype=jnp.int32)[None, None, :] < edge_count[:, :, None]
    return jnp.where(live, values, jnp.zeros_like(values))
```

```python
import jax
import jax.numpy as jnp
from jax import lax
from jax.experimental import pallas as pl
from jax.experimental.pallas import tpu as pltpu
from jax.sharding import PartitionSpec as P

STEPS = 2
PIECES = 2
MESH = pl.DeviceIdType.MESH


def split_parts(value, parts_ref, index):
    rest = value
    for piece in range(PIECES):
        part = rest.astype(jnp.bfloat16)
        parts_ref[index, piece] = part
        if piece + 1 < PIECES:
            rest = rest - part.astype(jnp.float32)


def picked_rows(indices, parts_ref, index, width):
    count = indices.shape[1]
    down = jnp.transpose(jnp.broadcast_to(indices, (count, count)))
    halves = [
        (down == lax.broadcasted_iota(jnp.int32, (count, count), 1) + first).astype(jnp.float32)
        for first in range(0, width, count)
    ]
    chosen = jnp.concatenate(halves, axis=1).astype(jnp.bfloat16)
    total = jnp.dot(chosen, parts_ref[index, 0], preferred_element_type=jnp.float32)
    for piece in range(1, PIECES):
        total += jnp.dot(chosen, parts_ref[index, piece], preferred_element_type=jnp.float32)
    return total


def kernel(
    x_hbm, z_hbm, src_ref, dst_ref, count_ref, out_ref,
    x_vmem, z_vmem, x_parts, z_parts, index_out, x_index, z_index, x_rows, z_rows,
    local_sem, index_send, x_index_sem, z_index_sem, x_send, z_send, x_recv, z_recv,
):
    row, col = lax.axis_index("row"), lax.axis_index("col")
    n_row, n_col = lax.axis_size("row"), lax.axis_size("col")
    slots = src_ref.shape[2]
    width = x_parts.shape[2]
    cells = 2
    offsets = cells + STEPS - 1

    x_copy = pltpu.make_async_copy(x_hbm, x_vmem, local_sem.at[0])
    z_copy = pltpu.make_async_copy(z_hbm, z_vmem, local_sem.at[1])
    x_copy.start()
    z_copy.start()

    x_owner = [lax.rem(col + cells * row + o, n_col) for o in range(offsets)]
    x_reader = [lax.rem(col - cells * row - o + 2 * n_col, n_col) for o in range(offsets)]
    half = col // cells
    z_owner = [lax.rem(row + half + d, n_row) for d in range(2)]
    z_reader = [lax.rem(row - half - d + 2 * n_row, n_row) for d in range(2)]
    x_self = [x_owner[o] == col for o in range(offsets)]
    z_self = [z_owner[d] == row for d in range(2)]

    barrier = pltpu.get_barrier_semaphore()
    links = [((row, x_owner[o]), (row, x_reader[o]), x_self[o]) for o in range(offsets)]
    links += [((z_owner[d], col), (z_reader[d], col), z_self[d]) for d in range(2)]
    for owner, reader, own in links:
        @pl.when(jnp.logical_not(own))
        def _():
            pl.semaphore_signal(barrier, inc=1, device_id=owner, device_id_type=MESH)
            pl.semaphore_signal(barrier, inc=1, device_id=reader, device_id_type=MESH)

    index_out[0, :, :slots] = src_ref[0]
    index_out[0, :, slots:] = src_ref[1]
    index_out[1, :, :slots] = dst_ref[0]
    index_out[1, :, slots:] = dst_ref[1]

    pl.semaphore_wait(barrier, sum(jnp.where(own, 0, 2) for _, _, own in links))

    def x_index_copy(o):
        return pltpu.make_async_remote_copy(
            src_ref=index_out.at[0], dst_ref=x_index.at[o], send_sem=index_send.at[o], recv_sem=x_index_sem.at[o],
            device_id=(row, x_owner[o]), device_id_type=MESH)

    def z_index_copy(d):
        return pltpu.make_async_remote_copy(
            src_ref=index_out.at[1], dst_ref=z_index.at[d], send_sem=index_send.at[offsets + d], recv_sem=z_index_sem.at[d],
            device_id=(z_owner[d], col), device_id_type=MESH)

    for o in range(offsets):
        @pl.when(jnp.logical_not(x_self[o]))
        def _(o=o):
            x_index_copy(o).start()

        @pl.when(x_self[o])
        def _(o=o):
            x_index[o] = index_out[0]
    for d in range(2):
        @pl.when(jnp.logical_not(z_self[d]))
        def _(d=d):
            z_index_copy(d).start()

        @pl.when(z_self[d])
        def _(d=d):
            z_index[d] = index_out[1]

    x_copy.wait()
    for c in range(cells):
        split_parts(x_vmem[c * width:(c + 1) * width, :], x_parts, c)
    z_copy.wait()
    for b in range(cells):
        split_parts(jnp.transpose(z_vmem[b * width:(b + 1) * width, :]), z_parts, b)

    low = lax.broadcasted_iota(jnp.int32, (1, 2 * slots), 1) < slots
    for o in range(offsets):
        @pl.when(jnp.logical_not(x_self[o]))
        def _(o=o):
            x_index_copy(o).wait_recv()
    first, second, third = (x_index[o] for o in range(offsets))
    turned = pltpu.roll(second, slots, 1)
    x_wanted = [jnp.where(low, first, turned), jnp.where(low, turned, third)]

    def x_copy_out(c, s):
        return pltpu.make_async_remote_copy(
            src_ref=x_rows.at[0, c, s], dst_ref=x_rows.at[1, c, s], send_sem=x_send.at[c, s], recv_sem=x_recv.at[c, s],
            device_id=(row, x_reader[c + s]), device_id_type=MESH)

    for c in range(cells):
        x_rows[0, c] = picked_rows(x_wanted[c], x_parts, c, width).reshape(STEPS, slots, width)
        for s in range(STEPS):
            @pl.when(jnp.logical_not(x_self[c + s]))
            def _(c=c, s=s):
                x_copy_out(c, s).start()

    for d in range(2):
        @pl.when(jnp.logical_not(z_self[d]))
        def _(d=d):
            z_index_copy(d).wait_recv()
    odd = lax.rem(col, 2)
    near, far = z_index[0], z_index[1]
    mixed = jnp.where(low, near, far)
    is_odd = jnp.broadcast_to(odd, (1, 2 * slots)) == 1
    z_wanted = [
        jnp.where(is_odd, pltpu.roll(far, slots, 1), mixed),
        jnp.where(is_odd, mixed, pltpu.roll(near, slots, 1)),
    ]

    def z_target(b, s):
        block = lax.rem(cells * row + b - col - s + 2 * n_col, n_col)
        return block // cells, lax.rem(block, cells)

    def z_copy_out(b, s):
        target, c = z_target(b, s)
        return pltpu.make_async_remote_copy(
            src_ref=z_rows.at[0, b, s], dst_ref=z_rows.at[1, c, s], send_sem=z_send.at[b, s], recv_sem=z_recv.at[c, s],
            device_id=(target, col), device_id_type=MESH)

    for b in range(cells):
        z_rows[0, b] = picked_rows(z_wanted[b], z_parts, b, width).reshape(STEPS, slots, width)
        for s in range(STEPS):
            @pl.when(z_target(b, s)[0] != row)
            def _(b=b, s=s):
                z_copy_out(b, s).start()

    def z_arrival(c, s):
        return pltpu.make_async_remote_copy(
            src_ref=z_rows.at[0, 0, s], dst_ref=z_rows.at[1, c, s], send_sem=z_send.at[0, s], recv_sem=z_recv.at[c, s],
            device_id=(row, col), device_id_type=MESH)

    for c in range(cells):
        total = None
        for s in range(STEPS):
            block = lax.rem(col + cells * row + c + s, n_col)
            z_own = block // cells == row

            @pl.when(jnp.logical_not(x_self[c + s]))
            def _(c=c, s=s):
                x_copy_out(c, s).wait_recv()

            @pl.when(jnp.logical_not(z_own))
            def _(c=c, s=s):
                z_arrival(c, s).wait_recv()

            x_side = jnp.where(x_self[c + s], 0, 1)
            z_side = jnp.where(z_own, 0, 1)
            z_slot = jnp.where(z_own, lax.rem(block, cells), c)
            term = x_rows[x_side, c, s] * z_rows[z_side, z_slot, s]
            total = term if total is None else total + term
        folded = total[:, :slots]
        for at in range(slots, width, slots):
            folded = folded + total[:, at:at + slots]
        values = jnp.sum(jnp.transpose(folded), axis=0, keepdims=True)
        live = lax.broadcasted_iota(jnp.int32, (1, slots), 1) < count_ref[c]
        out_ref[c] = jnp.where(live, values, jnp.zeros_like(values))

    for o in range(offsets):
        @pl.when(jnp.logical_not(x_self[o]))
        def _(o=o):
            x_index_copy(o).wait_send()
    for d in range(2):
        @pl.when(jnp.logical_not(z_self[d]))
        def _(d=d):
            z_index_copy(d).wait_send()
    for c in range(cells):
        for s in range(STEPS):
            @pl.when(jnp.logical_not(x_self[c + s]))
            def _(c=c, s=s):
                x_copy_out(c, s).wait_send()

            @pl.when(z_target(c, s)[0] != row)
            def _(c=c, s=s):
                z_copy_out(c, s).wait_send()


def body(x_iterate, z_inverse, edge_src, edge_dst, edge_count):
    height, width = x_iterate.shape
    cells, _, slots = edge_src.shape
    return pl.pallas_call(
        kernel,
        out_shape=jax.ShapeDtypeStruct((cells, 1, slots), jnp.float32),
        in_specs=[
            pl.BlockSpec(memory_space=pltpu.HBM),
            pl.BlockSpec(memory_space=pltpu.HBM),
            pl.BlockSpec(memory_space=pltpu.VMEM),
            pl.BlockSpec(memory_space=pltpu.VMEM),
            pl.BlockSpec(memory_space=pltpu.SMEM),
        ],
        out_specs=pl.BlockSpec(memory_space=pltpu.VMEM),
        scratch_shapes=[
            pltpu.VMEM((height, width), jnp.float32),
            pltpu.VMEM((height, width), jnp.float32),
            pltpu.VMEM((cells, PIECES, width, width), jnp.bfloat16),
            pltpu.VMEM((cells, PIECES, width, width), jnp.bfloat16),
            pltpu.VMEM((2, 1, cells * slots), jnp.int32),
            pltpu.VMEM((cells + STEPS - 1, 1, cells * slots), jnp.int32),
            pltpu.VMEM((2, 1, cells * slots), jnp.int32),
            pltpu.VMEM((2, cells, STEPS, slots, width), jnp.float32),
            pltpu.VMEM((2, cells, STEPS, slots, width), jnp.float32),
            pltpu.SemaphoreType.DMA((2,)),
            pltpu.SemaphoreType.DMA((cells + STEPS + 1,)),
            pltpu.SemaphoreType.DMA((cells + STEPS - 1,)),
            pltpu.SemaphoreType.DMA((2,)),
            pltpu.SemaphoreType.DMA((cells, STEPS)),
            pltpu.SemaphoreType.DMA((cells, STEPS)),
            pltpu.SemaphoreType.DMA((cells, STEPS)),
            pltpu.SemaphoreType.DMA((cells, STEPS)),
        ],
        compiler_params=pltpu.CompilerParams(collective_id=0, has_side_effects=True),
        name="schur_row",
    )(x_iterate, z_inverse, edge_src, edge_dst, edge_count.reshape(cells))


def solution(mesh):
    return jax.shard_map(
        body,
        mesh=mesh,
        in_specs=(
            P("row", "col"),
            P("row", "col"),
            P("row", "col", None),
            P("row", "col", None),
            P("row", "col"),
        ),
        out_specs=P("row", "col", None),
        check_vma=False,
    )
```

```python
import jax
import jax.numpy as jnp
from jax import lax
from jax.experimental import pallas as pl
from jax.experimental.pallas import tpu as pltpu
from jax.sharding import PartitionSpec as P

STEPS = 2
PIECES = 2
MESH = pl.DeviceIdType.MESH


def split_parts(value, parts_ref, index):
    rest = value
    for piece in range(PIECES):
        part = rest.astype(jnp.bfloat16)
        parts_ref[index, piece] = part
        if piece + 1 < PIECES:
            rest = rest - part.astype(jnp.float32)


def picked_rows(indices, parts_ref, index, width):
    count = indices.shape[1]
    down = jnp.transpose(jnp.broadcast_to(indices, (count, count)))
    halves = [
        (down == lax.broadcasted_iota(jnp.int32, (count, count), 1) + first).astype(jnp.float32)
        for first in range(0, width, count)
    ]
    chosen = jnp.concatenate(halves, axis=1).astype(jnp.bfloat16)
    total = jnp.dot(chosen, parts_ref[index, 0], preferred_element_type=jnp.float32)
    for piece in range(1, PIECES):
        total += jnp.dot(chosen, parts_ref[index, piece], preferred_element_type=jnp.float32)
    return total


def kernel(
    x_hbm, z_hbm, src_hbm, dst_hbm, out_ref,
    x_vmem, z_vmem, x_parts, z_parts, index_in, index_out, x_index, z_index, x_rows, z_rows,
    local_sem, index_send, x_index_sem, z_index_sem, x_send, z_send, x_recv, z_recv,
):
    row, col = lax.axis_index("row"), lax.axis_index("col")
    n_row, n_col = lax.axis_size("row"), lax.axis_size("col")
    slots = src_hbm.shape[2]
    width = x_parts.shape[2]
    cells = 2
    offsets = cells + STEPS - 1

    x_copy = pltpu.make_async_copy(x_hbm, x_vmem, local_sem.at[0])
    z_copy = pltpu.make_async_copy(z_hbm, z_vmem, local_sem.at[1])

    x_owner = [lax.rem(col + cells * row + o, n_col) for o in range(offsets)]
    x_reader = [lax.rem(col - cells * row - o + 2 * n_col, n_col) for o in range(offsets)]
    half = col // cells
    z_owner = [lax.rem(row + half + d, n_row) for d in range(2)]
    z_reader = [lax.rem(row - half - d + 2 * n_row, n_row) for d in range(2)]
    x_self = [x_owner[o] == col for o in range(offsets)]
    z_self = [z_owner[d] == row for d in range(2)]

    barrier = pltpu.get_barrier_semaphore()
    links = [((row, x_reader[o]), x_self[o]) for o in range(offsets)]
    links += [((z_reader[d], col), z_self[d]) for d in range(2)]
    for reader, own in links:
        @pl.when(jnp.logical_not(own))
        def _():
            pl.semaphore_signal(barrier, inc=1, device_id=reader, device_id_type=MESH)

    src_copy = pltpu.make_async_copy(src_hbm, index_in.at[0], local_sem.at[2])
    dst_copy = pltpu.make_async_copy(dst_hbm, index_in.at[1], local_sem.at[3])
    src_copy.start()
    dst_copy.start()
    x_copy.start()
    z_copy.start()
    src_copy.wait()
    dst_copy.wait()
    for which in range(2):
        index_out[which, :, :slots] = index_in[which, 0]
        index_out[which, :, slots:] = index_in[which, 1]

    pl.semaphore_wait(barrier, sum(jnp.where(own, 0, 1) for _, own in links))

    def x_index_copy(o):
        return pltpu.make_async_remote_copy(
            src_ref=index_out.at[0], dst_ref=x_index.at[o], send_sem=index_send.at[o], recv_sem=x_index_sem.at[o],
            device_id=(row, x_owner[o]), device_id_type=MESH)

    def z_index_copy(d):
        return pltpu.make_async_remote_copy(
            src_ref=index_out.at[1], dst_ref=z_index.at[d], send_sem=index_send.at[offsets + d], recv_sem=z_index_sem.at[d],
            device_id=(z_owner[d], col), device_id_type=MESH)

    for o in range(offsets):
        @pl.when(jnp.logical_not(x_self[o]))
        def _(o=o):
            x_index_copy(o).start()

        @pl.when(x_self[o])
        def _(o=o):
            x_index[o] = index_out[0]
    for d in range(2):
        @pl.when(jnp.logical_not(z_self[d]))
        def _(d=d):
            z_index_copy(d).start()

        @pl.when(z_self[d])
        def _(d=d):
            z_index[d] = index_out[1]

    x_copy.wait()
    for c in range(cells):
        split_parts(x_vmem[c * width:(c + 1) * width, :], x_parts, c)
    z_copy.wait()
    for b in range(cells):
        split_parts(jnp.transpose(z_vmem[b * width:(b + 1) * width, :]), z_parts, b)

    low = lax.broadcasted_iota(jnp.int32, (1, 2 * slots), 1) < slots
    for o in range(offsets):
        @pl.when(jnp.logical_not(x_self[o]))
        def _(o=o):
            x_index_copy(o).wait_recv()
    first, second, third = (x_index[o] for o in range(offsets))
    turned = pltpu.roll(second, slots, 1)
    x_wanted = [jnp.where(low, first, turned), jnp.where(low, turned, third)]

    def x_copy_out(c, s):
        return pltpu.make_async_remote_copy(
            src_ref=x_rows.at[0, c, s], dst_ref=x_rows.at[1, c, s], send_sem=x_send.at[c, s], recv_sem=x_recv.at[c, s],
            device_id=(row, x_reader[c + s]), device_id_type=MESH)

    for c in range(cells):
        x_rows[0, c] = picked_rows(x_wanted[c], x_parts, c, width).reshape(STEPS, slots, width)
        for s in range(STEPS):
            @pl.when(jnp.logical_not(x_self[c + s]))
            def _(c=c, s=s):
                x_copy_out(c, s).start()

    for d in range(2):
        @pl.when(jnp.logical_not(z_self[d]))
        def _(d=d):
            z_index_copy(d).wait_recv()
    odd = lax.rem(col, 2)
    near, far = z_index[0], z_index[1]
    mixed = jnp.where(low, near, far)
    is_odd = jnp.broadcast_to(odd, (1, 2 * slots)) == 1
    z_wanted = [
        jnp.where(is_odd, pltpu.roll(far, slots, 1), mixed),
        jnp.where(is_odd, mixed, pltpu.roll(near, slots, 1)),
    ]

    def z_target(b, s):
        block = lax.rem(cells * row + b - col - s + 2 * n_col, n_col)
        return block // cells, lax.rem(block, cells)

    def z_copy_out(b, s):
        target, c = z_target(b, s)
        return pltpu.make_async_remote_copy(
            src_ref=z_rows.at[0, b, s], dst_ref=z_rows.at[1, c, s], send_sem=z_send.at[b, s], recv_sem=z_recv.at[c, s],
            device_id=(target, col), device_id_type=MESH)

    for b in range(cells):
        z_rows[0, b] = picked_rows(z_wanted[b], z_parts, b, width).reshape(STEPS, slots, width)
        for s in range(STEPS):
            @pl.when(z_target(b, s)[0] != row)
            def _(b=b, s=s):
                z_copy_out(b, s).start()

    def z_arrival(c, s):
        return pltpu.make_async_remote_copy(
            src_ref=z_rows.at[0, 0, s], dst_ref=z_rows.at[1, c, s], send_sem=z_send.at[0, s], recv_sem=z_recv.at[c, s],
            device_id=(row, col), device_id_type=MESH)

    for c in range(cells):
        total = None
        for s in range(STEPS):
            block = lax.rem(col + cells * row + c + s, n_col)
            z_own = block // cells == row

            @pl.when(jnp.logical_not(x_self[c + s]))
            def _(c=c, s=s):
                x_copy_out(c, s).wait_recv()

            @pl.when(jnp.logical_not(z_own))
            def _(c=c, s=s):
                z_arrival(c, s).wait_recv()

            x_side = jnp.where(x_self[c + s], 0, 1)
            z_side = jnp.where(z_own, 0, 1)
            z_slot = jnp.where(z_own, lax.rem(block, cells), c)
            term = x_rows[x_side, c, s] * z_rows[z_side, z_slot, s]
            total = term if total is None else total + term
        folded = total[:, :slots]
        for at in range(slots, width, slots):
            folded = folded + total[:, at:at + slots]
        values = jnp.sum(jnp.transpose(folded), axis=0, keepdims=True)
        out_ref[c] = values

    for o in range(offsets):
        @pl.when(jnp.logical_not(x_self[o]))
        def _(o=o):
            x_index_copy(o).wait_send()
    for d in range(2):
        @pl.when(jnp.logical_not(z_self[d]))
        def _(d=d):
            z_index_copy(d).wait_send()
    for c in range(cells):
        for s in range(STEPS):
            @pl.when(jnp.logical_not(x_self[c + s]))
            def _(c=c, s=s):
                x_copy_out(c, s).wait_send()

            @pl.when(z_target(c, s)[0] != row)
            def _(c=c, s=s):
                z_copy_out(c, s).wait_send()


def body(x_iterate, z_inverse, edge_src, edge_dst, edge_count):
    height, width = x_iterate.shape
    cells, _, slots = edge_src.shape
    values = pl.pallas_call(
        kernel,
        out_shape=jax.ShapeDtypeStruct((cells, 1, slots), jnp.float32),
        in_specs=[
            pl.BlockSpec(memory_space=pltpu.HBM),
            pl.BlockSpec(memory_space=pltpu.HBM),
            pl.BlockSpec(memory_space=pltpu.HBM),
            pl.BlockSpec(memory_space=pltpu.HBM),
        ],
        out_specs=pl.BlockSpec(memory_space=pltpu.VMEM),
        scratch_shapes=[
            pltpu.VMEM((height, width), jnp.float32),
            pltpu.VMEM((height, width), jnp.float32),
            pltpu.VMEM((cells, PIECES, width, width), jnp.bfloat16),
            pltpu.VMEM((cells, PIECES, width, width), jnp.bfloat16),
            pltpu.VMEM((2, cells, 1, slots), jnp.int32),
            pltpu.VMEM((2, 1, cells * slots), jnp.int32),
            pltpu.VMEM((cells + STEPS - 1, 1, cells * slots), jnp.int32),
            pltpu.VMEM((2, 1, cells * slots), jnp.int32),
            pltpu.VMEM((2, cells, STEPS, slots, width), jnp.float32),
            pltpu.VMEM((2, cells, STEPS, slots, width), jnp.float32),
            pltpu.SemaphoreType.DMA((4,)),
            pltpu.SemaphoreType.DMA((cells + STEPS + 1,)),
            pltpu.SemaphoreType.DMA((cells + STEPS - 1,)),
            pltpu.SemaphoreType.DMA((2,)),
            pltpu.SemaphoreType.DMA((cells, STEPS)),
            pltpu.SemaphoreType.DMA((cells, STEPS)),
            pltpu.SemaphoreType.DMA((cells, STEPS)),
            pltpu.SemaphoreType.DMA((cells, STEPS)),
        ],
        compiler_params=pltpu.CompilerParams(collective_id=0, has_side_effects=True, vmem_limit_bytes=8 * 2**20),
        name="schur_row",
    )(*(pltpu.with_memory_space_constraint(operand, pltpu.HBM) for operand in (x_iterate, z_inverse, edge_src, edge_dst)))
    live = lax.broadcasted_iota(jnp.int32, values.shape, 2) < edge_count[:, :, None]
    return jnp.where(live, values, jnp.zeros_like(values))


def solution(mesh):
    return jax.shard_map(
        body,
        mesh=mesh,
        in_specs=(
            P("row", "col"),
            P("row", "col"),
            P("row", "col", None),
            P("row", "col", None),
            P("row", "col"),
        ),
        out_specs=P("row", "col", None),
        check_vma=False,
    )
```

```python
import jax
import jax.numpy as jnp
from jax import lax
from jax.experimental import pallas as pl
from jax.experimental.pallas import tpu as pltpu
from jax.sharding import PartitionSpec as P

STEPS = 2
PIECES = 2
MESH = pl.DeviceIdType.MESH


def split_parts(value, parts_ref, index):
    rest = value
    for piece in range(PIECES):
        part = rest.astype(jnp.bfloat16)
        parts_ref[index, piece] = part
        if piece + 1 < PIECES:
            rest = rest - part.astype(jnp.float32)


def picked_rows(indices, parts_ref, index, width):
    count = indices.shape[1]
    down = jnp.transpose(jnp.broadcast_to(indices, (count, count)))
    halves = [
        (down == lax.broadcasted_iota(jnp.int32, (count, count), 1) + first).astype(jnp.float32)
        for first in range(0, width, count)
    ]
    chosen = jnp.concatenate(halves, axis=1).astype(jnp.bfloat16)
    total = jnp.dot(chosen, parts_ref[index, 0], preferred_element_type=jnp.float32)
    for piece in range(1, PIECES):
        total += jnp.dot(chosen, parts_ref[index, piece], preferred_element_type=jnp.float32)
    return total


def kernel(
    x_hbm, z_hbm, src_hbm, dst_hbm, out_ref,
    x_vmem, z_vmem, x_parts, z_parts, index_in, index_out, x_index, z_index, x_rows, z_rows, given, taken,
    local_sem, index_send, x_index_sem, z_index_sem, x_send, z_send, x_recv, z_recv, given_sem,
):
    row, col = lax.axis_index("row"), lax.axis_index("col")
    n_row, n_col = lax.axis_size("row"), lax.axis_size("col")
    slots = src_hbm.shape[2]
    width = x_parts.shape[2]
    cells = 2
    offsets = cells + STEPS - 1

    x_copy = pltpu.make_async_copy(x_hbm, x_vmem, local_sem.at[0])
    z_copy = pltpu.make_async_copy(z_hbm, z_vmem, local_sem.at[1])

    x_owner = [lax.rem(col + cells * row + o, n_col) for o in range(offsets)]
    x_reader = [lax.rem(col - cells * row - o + 2 * n_col, n_col) for o in range(offsets)]
    half = col // cells
    z_owner = [lax.rem(row + half + d, n_row) for d in range(2)]
    z_reader = [lax.rem(row - half - d + 2 * n_row, n_row) for d in range(2)]
    x_self = [x_owner[o] == col for o in range(offsets)]

    layer, chips = n_row // 2, n_col // 4
    twin = lax.rem(row + layer, n_row)

    def moved(reader_row, reader_col):
        diagonal = lax.rem(reader_row, layer) + lax.rem(reader_col, n_col // 2) // 2
        return jnp.where(diagonal == chips - 1, 0, lax.rem(reader_col // (n_col // 2) + diagonal // chips, 2))

    x_row = [lax.rem(row + layer * moved(row, x_reader[o]), n_row) for o in range(offsets)]
    x_sends = [jnp.logical_or(x_row[o] != row, jnp.logical_not(x_self[o])) for o in range(offsets)]
    away = moved(row, col)
    for_row = lax.rem(row + layer * away, n_row)
    work_block = [lax.rem(col + cells * for_row + o, n_col) for o in range(offsets)]
    x_here = [jnp.logical_and(away == 0, work_block[o] == col) for o in range(offsets)]
    z_here = [work_block[o] // cells == row for o in range(offsets)]
    z_self = [z_owner[d] == row for d in range(2)]

    barrier = pltpu.get_barrier_semaphore()
    links = [((row, x_reader[o]), x_self[o]) for o in range(offsets)]
    links += [((z_reader[d], col), z_self[d]) for d in range(2)]
    pl.semaphore_signal(barrier, inc=1, device_id=(twin, col), device_id_type=MESH)
    for reader, own in links:
        @pl.when(jnp.logical_not(own))
        def _():
            pl.semaphore_signal(barrier, inc=1, device_id=reader, device_id_type=MESH)

    src_copy = pltpu.make_async_copy(src_hbm, index_in.at[0], local_sem.at[2])
    dst_copy = pltpu.make_async_copy(dst_hbm, index_in.at[1], local_sem.at[3])
    src_copy.start()
    dst_copy.start()
    x_copy.start()
    z_copy.start()
    src_copy.wait()
    dst_copy.wait()
    for which in range(2):
        index_out[which, :, :slots] = index_in[which, 0]
        index_out[which, :, slots:] = index_in[which, 1]

    pl.semaphore_wait(barrier, 1 + sum(jnp.where(own, 0, 1) for _, own in links))

    def x_index_copy(o):
        return pltpu.make_async_remote_copy(
            src_ref=index_out.at[0], dst_ref=x_index.at[o], send_sem=index_send.at[o], recv_sem=x_index_sem.at[o],
            device_id=(row, x_owner[o]), device_id_type=MESH)

    def z_index_copy(d):
        return pltpu.make_async_remote_copy(
            src_ref=index_out.at[1], dst_ref=z_index.at[d], send_sem=index_send.at[offsets + d], recv_sem=z_index_sem.at[d],
            device_id=(z_owner[d], col), device_id_type=MESH)

    for o in range(offsets):
        @pl.when(jnp.logical_not(x_self[o]))
        def _(o=o):
            x_index_copy(o).start()

        @pl.when(x_self[o])
        def _(o=o):
            x_index[o] = index_out[0]
    for d in range(2):
        @pl.when(jnp.logical_not(z_self[d]))
        def _(d=d):
            z_index_copy(d).start()

        @pl.when(z_self[d])
        def _(d=d):
            z_index[d] = index_out[1]

    x_copy.wait()
    for c in range(cells):
        split_parts(x_vmem[c * width:(c + 1) * width, :], x_parts, c)
    z_copy.wait()
    for b in range(cells):
        split_parts(jnp.transpose(z_vmem[b * width:(b + 1) * width, :]), z_parts, b)

    low = lax.broadcasted_iota(jnp.int32, (1, 2 * slots), 1) < slots
    for d in range(2):
        @pl.when(jnp.logical_not(z_self[d]))
        def _(d=d):
            z_index_copy(d).wait_recv()
    odd = lax.rem(col, 2)
    near, far = z_index[0], z_index[1]
    mixed = jnp.where(low, near, far)
    is_odd = jnp.broadcast_to(odd, (1, 2 * slots)) == 1
    z_wanted = [
        jnp.where(is_odd, pltpu.roll(far, slots, 1), mixed),
        jnp.where(is_odd, mixed, pltpu.roll(near, slots, 1)),
    ]

    def z_target(b, s):
        block = lax.rem(cells * row + b - col - s + 2 * n_col, n_col)
        reader = block // cells
        return lax.rem(reader + layer * moved(reader, col), n_row), lax.rem(block, cells)

    def z_copy_out(b, s):
        target, c = z_target(b, s)
        return pltpu.make_async_remote_copy(
            src_ref=z_rows.at[0, b, s], dst_ref=z_rows.at[1, c, s], send_sem=z_send.at[b, s], recv_sem=z_recv.at[c, s],
            device_id=(target, col), device_id_type=MESH)

    for b in range(cells):
        z_rows[0, b] = picked_rows(z_wanted[b], z_parts, b, width).reshape(STEPS, slots, width)
        for s in range(STEPS):
            @pl.when(z_target(b, s)[0] != row)
            def _(b=b, s=s):
                z_copy_out(b, s).start()

    for o in range(offsets):
        @pl.when(jnp.logical_not(x_self[o]))
        def _(o=o):
            x_index_copy(o).wait_recv()
    first, second, third = (x_index[o] for o in range(offsets))
    turned = pltpu.roll(second, slots, 1)
    x_wanted = [jnp.where(low, first, turned), jnp.where(low, turned, third)]

    def x_copy_out(c, s):
        return pltpu.make_async_remote_copy(
            src_ref=x_rows.at[0, c, s], dst_ref=x_rows.at[1, c, s], send_sem=x_send.at[c, s], recv_sem=x_recv.at[c, s],
            device_id=(x_row[c + s], x_reader[c + s]), device_id_type=MESH)

    for c in range(cells):
        x_rows[0, c] = picked_rows(x_wanted[c], x_parts, c, width).reshape(STEPS, slots, width)
        for s in range(STEPS):
            @pl.when(x_sends[c + s])
            def _(c=c, s=s):
                x_copy_out(c, s).start()

    def z_arrival(c, s):
        return pltpu.make_async_remote_copy(
            src_ref=z_rows.at[0, 0, s], dst_ref=z_rows.at[1, c, s], send_sem=z_send.at[0, s], recv_sem=z_recv.at[c, s],
            device_id=(row, col), device_id_type=MESH)

    for c in range(cells):
        total = None
        for s in range(STEPS):
            u = c + s

            @pl.when(jnp.logical_not(x_here[u]))
            def _(c=c, s=s):
                x_copy_out(c, s).wait_recv()

            @pl.when(jnp.logical_not(z_here[u]))
            def _(c=c, s=s):
                z_arrival(c, s).wait_recv()

            x_side = jnp.where(x_here[u], 0, 1)
            z_side = jnp.where(z_here[u], 0, 1)
            z_slot = jnp.where(z_here[u], lax.rem(work_block[u], cells), c)
            term = x_rows[x_side, c, s] * z_rows[z_side, z_slot, s]
            total = term if total is None else total + term
        folded = total[:, :slots]
        for at in range(slots, width, slots):
            folded = folded + total[:, at:at + slots]
        given[c] = jnp.sum(jnp.transpose(folded), axis=0, keepdims=True)

    given_copy = pltpu.make_async_remote_copy(
        src_ref=given, dst_ref=taken, send_sem=given_sem.at[0], recv_sem=given_sem.at[1],
        device_id=(twin, col), device_id_type=MESH)

    @pl.when(away == 1)
    def _():
        given_copy.start()

    for o in range(offsets):
        @pl.when(jnp.logical_not(x_self[o]))
        def _(o=o):
            x_index_copy(o).wait_send()
    for d in range(2):
        @pl.when(jnp.logical_not(z_self[d]))
        def _(d=d):
            z_index_copy(d).wait_send()
    for c in range(cells):
        for s in range(STEPS):
            @pl.when(x_sends[c + s])
            def _(c=c, s=s):
                x_copy_out(c, s).wait_send()

            @pl.when(z_target(c, s)[0] != row)
            def _(c=c, s=s):
                z_copy_out(c, s).wait_send()

    @pl.when(away == 1)
    def _():
        given_copy.wait()
        out_ref[...] = taken[...]

    @pl.when(away == 0)
    def _():
        out_ref[...] = given[...]


def body(x_iterate, z_inverse, edge_src, edge_dst, edge_count):
    height, width = x_iterate.shape
    cells, _, slots = edge_src.shape
    values = pl.pallas_call(
        kernel,
        out_shape=jax.ShapeDtypeStruct((cells, 1, slots), jnp.float32),
        in_specs=[
            pl.BlockSpec(memory_space=pltpu.HBM),
            pl.BlockSpec(memory_space=pltpu.HBM),
            pl.BlockSpec(memory_space=pltpu.HBM),
            pl.BlockSpec(memory_space=pltpu.HBM),
        ],
        out_specs=pl.BlockSpec(memory_space=pltpu.VMEM),
        scratch_shapes=[
            pltpu.VMEM((height, width), jnp.float32),
            pltpu.VMEM((height, width), jnp.float32),
            pltpu.VMEM((cells, PIECES, width, width), jnp.bfloat16),
            pltpu.VMEM((cells, PIECES, width, width), jnp.bfloat16),
            pltpu.VMEM((2, cells, 1, slots), jnp.int32),
            pltpu.VMEM((2, 1, cells * slots), jnp.int32),
            pltpu.VMEM((cells + STEPS - 1, 1, cells * slots), jnp.int32),
            pltpu.VMEM((2, 1, cells * slots), jnp.int32),
            pltpu.VMEM((2, cells, STEPS, slots, width), jnp.float32),
            pltpu.VMEM((2, cells, STEPS, slots, width), jnp.float32),
            pltpu.VMEM((cells, 1, slots), jnp.float32),
            pltpu.VMEM((cells, 1, slots), jnp.float32),
            pltpu.SemaphoreType.DMA((4,)),
            pltpu.SemaphoreType.DMA((cells + STEPS + 1,)),
            pltpu.SemaphoreType.DMA((cells + STEPS - 1,)),
            pltpu.SemaphoreType.DMA((2,)),
            pltpu.SemaphoreType.DMA((cells, STEPS)),
            pltpu.SemaphoreType.DMA((cells, STEPS)),
            pltpu.SemaphoreType.DMA((cells, STEPS)),
            pltpu.SemaphoreType.DMA((cells, STEPS)),
            pltpu.SemaphoreType.DMA((2,)),
        ],
        compiler_params=pltpu.CompilerParams(collective_id=0, has_side_effects=True, vmem_limit_bytes=8 * 2**20),
        name="schur_row",
    )(*(pltpu.with_memory_space_constraint(operand, pltpu.HBM) for operand in (x_iterate, z_inverse, edge_src, edge_dst)))
    live = lax.broadcasted_iota(jnp.int32, values.shape, 2) < edge_count[:, :, None]
    return jnp.where(live, values, jnp.zeros_like(values))


def solution(mesh):
    return jax.shard_map(
        body,
        mesh=mesh,
        in_specs=(
            P("row", "col"),
            P("row", "col"),
            P("row", "col", None),
            P("row", "col", None),
            P("row", "col"),
        ),
        out_specs=P("row", "col", None),
        check_vma=False,
    )
```

```python
import jax
import jax.numpy as jnp
from jax import lax
from jax.experimental import pallas as pl
from jax.experimental.pallas import tpu as pltpu
from jax.sharding import PartitionSpec as P

STEPS = 2
PIECES = 2
MESH = pl.DeviceIdType.MESH


def split_parts(value, parts_ref, *index):
    rest = value
    for piece in range(PIECES):
        part = rest.astype(jnp.bfloat16)
        parts_ref[(*index, piece)] = part
        if piece + 1 < PIECES:
            rest = rest - part.astype(jnp.float32)


def kernel(
    x_hbm, z_hbm, src_hbm, dst_hbm, out_ref,
    x_vmem, z_vmem, parts, index_in, index_out, wanted, rows_out, rows_in, given, taken,
    local_sem, index_send, index_recv, rows_send, rows_recv, given_sem,
):
    row, col = lax.axis_index("row"), lax.axis_index("col")
    n_row, n_col = lax.axis_size("row"), lax.axis_size("col")
    slots = src_hbm.shape[2]
    width = parts.shape[3]
    cells = 2
    layer, chips = n_row // 2, n_col // 4
    twin = lax.rem(row + layer, n_row)

    def moved(reader_row, reader_col):
        diagonal = lax.rem(reader_row, layer) + lax.rem(reader_col, n_col // 2) // 2
        return jnp.where(diagonal == chips - 1, 0, lax.rem(reader_col // (n_col // 2) + diagonal // chips, 2))

    def working(reader_row, reader_col):
        return lax.rem(reader_row + layer * moved(reader_row, reader_col), n_row)

    x_owner = [lax.rem(col + cells * row + u, n_col) for u in range(3)]
    x_reader = [lax.rem(col - cells * row - u + 2 * n_col, n_col) for u in range(3)]
    half = col // cells
    z_owner = [lax.rem(row + half + d, n_row) for d in range(2)]
    z_reader = [lax.rem(row - half - d + 2 * n_row, n_row) for d in range(2)]
    links = [((row, x_reader[u]), x_owner[u] == col) for u in range(3)]
    links += [((z_reader[d], col), z_owner[d] == row) for d in range(2)]
    barrier = pltpu.get_barrier_semaphore()
    pl.semaphore_signal(barrier, inc=1, device_id=(twin, col), device_id_type=MESH)
    for reader, own in links:
        @pl.when(jnp.logical_not(own))
        def _():
            pl.semaphore_signal(barrier, inc=1, device_id=reader, device_id_type=MESH)

    src_copy = pltpu.make_async_copy(src_hbm, index_in.at[0], local_sem.at[2])
    dst_copy = pltpu.make_async_copy(dst_hbm, index_in.at[1], local_sem.at[3])
    x_copy = pltpu.make_async_copy(x_hbm, x_vmem, local_sem.at[0])
    z_copy = pltpu.make_async_copy(z_hbm, z_vmem, local_sem.at[1])
    src_copy.start()
    dst_copy.start()
    x_copy.start()
    z_copy.start()
    src_copy.wait()
    dst_copy.wait()
    for which in range(2):
        index_out[which, :, :slots] = index_in[which, 0]
        index_out[which, :, slots:] = index_in[which, 1]
    pl.semaphore_wait(barrier, 1 + sum(jnp.where(own, 0, 1) for _, own in links))

    def owner_of(kind, c, s):
        block = lax.rem(col + cells * row + c + s, n_col)
        if kind == 0:
            return row, block, c
        return block // cells, col, lax.rem(block, cells)

    def index_copy(kind, c, s):
        orow, ocol, p = owner_of(kind, c, s)
        return pltpu.make_async_remote_copy(
            src_ref=index_out.at[kind], dst_ref=wanted.at[kind, p, s], send_sem=index_send.at[kind, c, s],
            recv_sem=index_recv.at[kind, p, s], device_id=(orow, ocol), device_id_type=MESH)

    def owner_self(kind, c, s):
        orow, ocol, _ = owner_of(kind, c, s)
        return jnp.logical_and(orow == row, ocol == col)

    tasks = [(k, c, s) for k in (1, 0) for c in range(cells) for s in range(STEPS)]
    for t in tasks:
        @pl.when(jnp.logical_not(owner_self(*t)))
        def _(t=t):
            index_copy(*t).start()

        @pl.when(owner_self(*t))
        def _(t=t):
            wanted[t[0], owner_of(*t)[2], t[2]] = index_out[t[0]]

    x_copy.wait()
    for c in range(cells):
        split_parts(x_vmem[c * width:(c + 1) * width, :], parts, 0, c)
    z_copy.wait()
    for b in range(cells):
        split_parts(jnp.transpose(z_vmem[b * width:(b + 1) * width, :]), parts, 1, b)

    def reader_of(kind, p, s):
        x_col = lax.rem(col - cells * row - p - s + 2 * n_col, n_col)
        block = lax.rem(cells * row + p - col - s + 2 * n_col, n_col)
        isz = kind == 1
        return jnp.where(isz, block // cells, row), jnp.where(isz, col, x_col), jnp.where(isz, lax.rem(block, cells), p)

    def rows_copy(kind, p, s):
        rrow, rcol, c = reader_of(kind, p, s)
        return pltpu.make_async_remote_copy(
            src_ref=rows_out.at[kind, p, s], dst_ref=rows_in.at[kind, c, s], send_sem=rows_send.at[kind, p, s],
            recv_sem=rows_recv.at[kind, c, s], device_id=(working(rrow, rcol), rcol), device_id_type=MESH)

    def stays(kind, p, s):
        rrow, rcol, c = reader_of(kind, p, s)
        return jnp.logical_and(working(rrow, rcol) == row, rcol == col)

    def handle(kind, p, s):
        rrow, rcol, c = reader_of(kind, p, s)

        @pl.when(jnp.logical_not(jnp.logical_and(rrow == row, rcol == col)))
        def _():
            pltpu.make_async_remote_copy(
                src_ref=index_out.at[0], dst_ref=wanted.at[kind, p, s], send_sem=index_send.at[kind, p, s],
                recv_sem=index_recv.at[kind, p, s], device_id=(row, col), device_id_type=MESH).wait_recv()

        both = wanted[kind, p, s]
        upper = jnp.broadcast_to(c, both.shape) == 1
        mine = jnp.where(upper, pltpu.roll(both, slots, 1), both)
        down = jnp.transpose(jnp.broadcast_to(mine, (2 * slots, 2 * slots)))[:slots]
        chosen = jnp.concatenate(
            [(down == lax.broadcasted_iota(jnp.int32, down.shape, 1) + first).astype(jnp.float32)
             for first in range(0, width, 2 * slots)], axis=1).astype(jnp.bfloat16)
        total = jnp.dot(chosen, parts[kind, p, 0], preferred_element_type=jnp.float32)
        for piece in range(1, PIECES):
            total += jnp.dot(chosen, parts[kind, p, piece], preferred_element_type=jnp.float32)
        rows_out[kind, p, s] = total

        @pl.when(jnp.logical_not(stays(kind, p, s)))
        def _():
            rows_copy(kind, p, s).start()

    for t in tasks:
        handle(*t)

    away = moved(row, col)
    for_row = working(row, col)
    for c in range(cells):
        total = None
        for s in range(STEPS):
            block = lax.rem(col + cells * for_row + c + s, n_col)
            x_here = jnp.logical_and(away == 0, block == col)
            z_here = block // cells == row
            for kind, here in ((0, x_here), (1, z_here)):
                @pl.when(jnp.logical_not(here))
                def _(kind=kind, c=c, s=s):
                    pltpu.make_async_remote_copy(
                        src_ref=rows_out.at[kind, c, s], dst_ref=rows_in.at[kind, c, s], send_sem=rows_send.at[kind, c, s],
                        recv_sem=rows_recv.at[kind, c, s], device_id=(row, col), device_id_type=MESH).wait_recv()
            slot = lax.rem(block, cells)
            x_side = jnp.where(x_here, rows_out[0, c, s], rows_in[0, c, s])
            z_side = jnp.where(z_here, rows_out[1, slot, s], rows_in[1, c, s])
            term = x_side * z_side
            total = term if total is None else total + term
        folded = total[:, :slots]
        for at in range(slots, width, slots):
            folded = folded + total[:, at:at + slots]
        given[c] = jnp.sum(jnp.transpose(folded), axis=0, keepdims=True)

    given_copy = pltpu.make_async_remote_copy(
        src_ref=given, dst_ref=taken, send_sem=given_sem.at[0], recv_sem=given_sem.at[1],
        device_id=(twin, col), device_id_type=MESH)

    @pl.when(away == 1)
    def _():
        given_copy.start()

    for t in tasks:
        @pl.when(jnp.logical_not(owner_self(*t)))
        def _(t=t):
            index_copy(*t).wait_send()

        @pl.when(jnp.logical_not(stays(*t)))
        def _(t=t):
            rows_copy(*t).wait_send()

    @pl.when(away == 1)
    def _():
        given_copy.wait()
        out_ref[...] = taken[...]

    @pl.when(away == 0)
    def _():
        out_ref[...] = given[...]


def body(x_iterate, z_inverse, edge_src, edge_dst, edge_count):
    height, width = x_iterate.shape
    cells, _, slots = edge_src.shape
    hbm = pl.BlockSpec(memory_space=pltpu.HBM)
    values = pl.pallas_call(
        kernel,
        out_shape=jax.ShapeDtypeStruct((cells, 1, slots), jnp.float32),
        in_specs=[hbm] * 4,
        out_specs=pl.BlockSpec(memory_space=pltpu.VMEM),
        scratch_shapes=[
            pltpu.VMEM((height, width), jnp.float32),
            pltpu.VMEM((height, width), jnp.float32),
            pltpu.VMEM((2, cells, PIECES, width, width), jnp.bfloat16),
            pltpu.VMEM((2, cells, 1, slots), jnp.int32),
            pltpu.VMEM((2, 1, cells * slots), jnp.int32),
            pltpu.VMEM((2, cells, STEPS, 1, cells * slots), jnp.int32),
            pltpu.VMEM((2, cells, STEPS, slots, width), jnp.float32),
            pltpu.VMEM((2, cells, STEPS, slots, width), jnp.float32),
            pltpu.VMEM((cells, 1, slots), jnp.float32),
            pltpu.VMEM((cells, 1, slots), jnp.float32),
            pltpu.SemaphoreType.DMA((4,)),
            pltpu.SemaphoreType.DMA((2, cells, STEPS)),
            pltpu.SemaphoreType.DMA((2, cells, STEPS)),
            pltpu.SemaphoreType.DMA((2, cells, STEPS)),
            pltpu.SemaphoreType.DMA((2, cells, STEPS)),
            pltpu.SemaphoreType.DMA((2,)),
        ],
        compiler_params=pltpu.CompilerParams(collective_id=0, has_side_effects=True, vmem_limit_bytes=8 * 2**20),
        name="schur_row",
    )(*(pltpu.with_memory_space_constraint(operand, pltpu.HBM) for operand in (x_iterate, z_inverse, edge_src, edge_dst)))
    live = lax.broadcasted_iota(jnp.int32, values.shape, 2) < edge_count[:, :, None]
    return jnp.where(live, values, jnp.zeros_like(values))


def solution(mesh):
    return jax.shard_map(
        body,
        mesh=mesh,
        in_specs=(
            P("row", "col"),
            P("row", "col"),
            P("row", "col", None),
            P("row", "col", None),
            P("row", "col"),
        ),
        out_specs=P("row", "col", None),
        check_vma=False,
    )
```

```python
import jax
import jax.numpy as jnp
from jax import lax
from jax.experimental import pallas as pl
from jax.experimental.pallas import tpu as pltpu
from jax.sharding import PartitionSpec as P

STEPS = 2
PIECES = 2
MESH = pl.DeviceIdType.MESH


def split_parts(value, parts_ref, *index):
    rest = value
    for piece in range(PIECES):
        part = rest.astype(jnp.bfloat16)
        parts_ref[(*index, piece)] = part
        if piece + 1 < PIECES:
            rest = rest - part.astype(jnp.float32)


def kernel(
    x_hbm, z_hbm, src_hbm, dst_hbm, out_ref,
    x_vmem, z_vmem, parts, index_in, index_out, wanted, rows_out, rows_in, held, near_out, given, taken,
    local_sem, index_send, index_recv, rows_send, rows_recv, push_sem, near_sem, given_sem,
):
    row, col = lax.axis_index("row"), lax.axis_index("col")
    n_row, n_col = lax.axis_size("row"), lax.axis_size("col")
    slots = src_hbm.shape[2]
    width = parts.shape[3]
    cells = 2
    layer, chips = n_row // 2, n_col // 4
    twin = lax.rem(row + layer, n_row)

    def moved(reader_row, reader_col):
        diagonal = lax.rem(reader_row, layer) + lax.rem(reader_col, n_col // 2) // 2
        return jnp.where(diagonal >= chips - 1, 0, reader_col // (n_col // 2))

    def working(reader_row, reader_col):
        return lax.rem(reader_row + layer * moved(reader_row, reader_col), n_row)

    def pushed(reader_row, reader_col, q):
        x, y = lax.rem(reader_row, layer), lax.rem(reader_col, n_col // 2) // 2
        early = jnp.logical_and(x + y < chips, reader_col < n_col // 2)
        return jnp.logical_and(jnp.logical_and(early, (x + 1) // 2 == 1), q == 1)

    core = lax.rem(col, 2)
    even = col - core
    for_row = working(row, col)
    gives_cell = 1 - core
    gives_to = lax.rem(col - cells * row - gives_cell - 1 + 2 * n_col, n_col)
    gives = pushed(row, gives_to, gives_cell)
    holds = pushed(for_row, even, core)
    giver = (for_row, lax.rem(even + cells * for_row + 1 + core, n_col))
    near = [pushed(row, even, c) for c in range(cells)]
    work_near = [pushed(for_row, even, c) for c in range(cells)]

    x_owner = [lax.rem(col + cells * row + u, n_col) for u in range(3)]
    x_reader = [lax.rem(col - cells * row - u + 2 * n_col, n_col) for u in range(3)]
    half = col // cells
    z_owner = [lax.rem(row + half + d, n_row) for d in range(2)]
    z_reader = [lax.rem(row - half - d + 2 * n_row, n_row) for d in range(2)]
    links = [((row, x_reader[u]), x_owner[u] == col) for u in range(3)]
    links += [((z_reader[d], col), z_owner[d] == row) for d in range(2)]
    barrier = pltpu.get_barrier_semaphore()
    for device in ((twin, col), (row, even + 1 - core), (twin, even + 1 - core)):
        pl.semaphore_signal(barrier, inc=1, device_id=device, device_id_type=MESH)

    @pl.when(holds)
    def _():
        pl.semaphore_signal(barrier, inc=1, device_id=giver, device_id_type=MESH)

    for reader, own in links:
        @pl.when(jnp.logical_not(own))
        def _():
            pl.semaphore_signal(barrier, inc=1, device_id=reader, device_id_type=MESH)

    src_copy = pltpu.make_async_copy(src_hbm, index_in.at[0], local_sem.at[2])
    dst_copy = pltpu.make_async_copy(dst_hbm, index_in.at[1], local_sem.at[3])
    x_copy = pltpu.make_async_copy(x_hbm, x_vmem, local_sem.at[0])
    z_copy = pltpu.make_async_copy(z_hbm, z_vmem, local_sem.at[1])
    src_copy.start()
    dst_copy.start()
    x_copy.start()
    z_copy.start()
    src_copy.wait()
    dst_copy.wait()
    for which in range(2):
        index_out[which, :, :slots] = index_in[which, 0]
        index_out[which, :, slots:] = index_in[which, 1]
    pl.semaphore_wait(barrier, 3 + jnp.where(gives, 1, 0) + sum(jnp.where(own, 0, 1) for _, own in links))

    def from_near(c, s):
        return jnp.logical_and(near[c], core == 1 - s)

    def owner_of(kind, c, s):
        block = lax.rem(col + cells * row + c + s, n_col)
        if kind == 0:
            close = from_near(c, s)
            return jnp.where(close, for_row, row), jnp.where(close, even + c, block), jnp.where(close, 0, c), jnp.where(close, 2, 0)
        return block // cells, col, lax.rem(block, cells), 1

    def index_copy(kind, c, s):
        orow, ocol, p, to = owner_of(kind, c, s)
        return pltpu.make_async_remote_copy(
            src_ref=index_out.at[kind], dst_ref=wanted.at[to, p, s], send_sem=index_send.at[kind, c, s],
            recv_sem=index_recv.at[to, p, s], device_id=(orow, ocol), device_id_type=MESH)

    def owner_self(kind, c, s):
        orow, ocol, _, _ = owner_of(kind, c, s)
        return jnp.logical_and(orow == row, ocol == col)

    tasks = [(k, c, s) for k in (1, 0) for c in range(cells) for s in range(STEPS)]
    for t in tasks:
        @pl.when(jnp.logical_not(owner_self(*t)))
        def _(t=t):
            index_copy(*t).start()

        @pl.when(owner_self(*t))
        def _(t=t):
            _, _, p, to = owner_of(*t)
            wanted[to, p, t[2]] = index_out[t[0]]

    x_copy.wait()
    push_copy = pltpu.make_async_remote_copy(
        src_ref=x_vmem.at[pl.ds(pl.multiple_of(gives_cell * width, width), width)], dst_ref=held, send_sem=push_sem.at[0],
        recv_sem=push_sem.at[1], device_id=(working(row, gives_to), gives_to + gives_cell), device_id_type=MESH)

    @pl.when(gives)
    def _():
        push_copy.start()

    for c in range(cells):
        split_parts(x_vmem[c * width:(c + 1) * width, :], parts, 0, c)
    z_copy.wait()
    for b in range(cells):
        split_parts(jnp.transpose(z_vmem[b * width:(b + 1) * width, :]), parts, 1, b)

    def reader_of(kind, p, s):
        x_col = lax.rem(col - cells * row - p - s + 2 * n_col, n_col)
        block = lax.rem(cells * row + p - col - s + 2 * n_col, n_col)
        isz = kind == 1
        return jnp.where(isz, block // cells, row), jnp.where(isz, col, x_col), jnp.where(isz, lax.rem(block, cells), p)

    def rows_copy(kind, p, s):
        rrow, rcol, c = reader_of(kind, p, s)
        return pltpu.make_async_remote_copy(
            src_ref=rows_out.at[kind, p, s], dst_ref=rows_in.at[kind, c, s], send_sem=rows_send.at[kind, p, s],
            recv_sem=rows_recv.at[kind, c, s], device_id=(working(rrow, rcol), rcol), device_id_type=MESH)

    def stays(kind, p, s):
        rrow, rcol, c = reader_of(kind, p, s)
        return jnp.logical_and(working(rrow, rcol) == row, rcol == col)

    def handle(kind, p, s):
        rrow, rcol, c = reader_of(kind, p, s)

        @pl.when(jnp.logical_not(jnp.logical_and(rrow == row, rcol == col)))
        def _():
            pltpu.make_async_remote_copy(
                src_ref=index_out.at[0], dst_ref=wanted.at[kind, p, s], send_sem=index_send.at[kind, p, s],
                recv_sem=index_recv.at[kind, p, s], device_id=(row, col), device_id_type=MESH).wait_recv()

        rows_out[kind, p, s] = gathered(wanted[kind, p, s], c, kind, p)

        @pl.when(jnp.logical_not(stays(kind, p, s)))
        def _():
            rows_copy(kind, p, s).start()

    def gathered(both, c, kind, p):
        upper = jnp.broadcast_to(c, both.shape) == 1
        mine = jnp.where(upper, pltpu.roll(both, slots, 1), both)
        down = jnp.transpose(jnp.broadcast_to(mine, (2 * slots, 2 * slots)))[:slots]
        chosen = jnp.concatenate(
            [(down == lax.broadcasted_iota(jnp.int32, down.shape, 1) + first).astype(jnp.float32)
             for first in range(0, width, 2 * slots)], axis=1).astype(jnp.bfloat16)
        total = jnp.dot(chosen, parts[kind, p, 0], preferred_element_type=jnp.float32)
        for piece in range(1, PIECES):
            total += jnp.dot(chosen, parts[kind, p, piece], preferred_element_type=jnp.float32)
        return total

    def skips(kind, p):
        return jnp.logical_and(gives, gives_cell == p) if kind == 0 else row < 0

    for t in tasks:
        @pl.when(jnp.logical_not(skips(*t[:2])))
        def _(t=t):
            handle(*t)

    def near_copy():
        s = core
        return pltpu.make_async_remote_copy(
            src_ref=near_out, dst_ref=rows_in.at[0, core, s], send_sem=near_sem.at[0], recv_sem=rows_recv.at[0, core, s],
            device_id=(row, even + 1 - core), device_id_type=MESH)

    @pl.when(holds)
    def _():
        push_copy.wait_recv()
        split_parts(held[...], parts, 2, 0)
        pltpu.make_async_remote_copy(
            src_ref=index_out.at[0], dst_ref=wanted.at[2, 0, core], send_sem=index_send.at[0, 0, 0],
            recv_sem=index_recv.at[2, 0, core], device_id=(row, col), device_id_type=MESH).wait_recv()
        near_out[...] = gathered(wanted[2, 0, core], core, 2, 0)
        near_copy().start()

        @pl.when(for_row != row)
        def _():
            pltpu.make_async_remote_copy(
                src_ref=index_out.at[0], dst_ref=wanted.at[2, 0, 1 - core], send_sem=index_send.at[0, 0, 0],
                recv_sem=index_recv.at[2, 0, 1 - core], device_id=(row, col), device_id_type=MESH).wait_recv()

        rows_in[0, core, 1 - core] = gathered(wanted[2, 0, 1 - core], core, 2, 0)

    away = moved(row, col)
    for c in range(cells):
        total = None
        for s in range(STEPS):
            block = lax.rem(col + cells * for_row + c + s, n_col)
            close = jnp.logical_and(work_near[c], core == 1 - s)
            x_here = jnp.logical_and(jnp.logical_and(away == 0, block == col), jnp.logical_not(close))
            x_got = jnp.logical_or(x_here, jnp.logical_and(close, core == c))
            z_here = block // cells == row
            for kind, here in ((0, x_got), (1, z_here)):
                @pl.when(jnp.logical_not(here))
                def _(kind=kind, c=c, s=s):
                    pltpu.make_async_remote_copy(
                        src_ref=rows_out.at[kind, c, s], dst_ref=rows_in.at[kind, c, s], send_sem=rows_send.at[kind, c, s],
                        recv_sem=rows_recv.at[kind, c, s], device_id=(row, col), device_id_type=MESH).wait_recv()
            slot = lax.rem(block, cells)
            x_side = jnp.where(x_here, rows_out[0, c, s], rows_in[0, c, s])
            z_side = jnp.where(z_here, rows_out[1, slot, s], rows_in[1, c, s])
            term = x_side * z_side
            total = term if total is None else total + term
        folded = total[:, :slots]
        for at in range(slots, width, slots):
            folded = folded + total[:, at:at + slots]
        given[c] = jnp.sum(jnp.transpose(folded), axis=0, keepdims=True)

    given_copy = pltpu.make_async_remote_copy(
        src_ref=given, dst_ref=taken, send_sem=given_sem.at[0], recv_sem=given_sem.at[1],
        device_id=(twin, col), device_id_type=MESH)

    @pl.when(away == 1)
    def _():
        given_copy.start()

    for t in tasks:
        @pl.when(jnp.logical_not(owner_self(*t)))
        def _(t=t):
            index_copy(*t).wait_send()

        @pl.when(jnp.logical_not(jnp.logical_or(stays(*t), skips(*t[:2]))))
        def _(t=t):
            rows_copy(*t).wait_send()

    @pl.when(gives)
    def _():
        push_copy.wait_send()

    @pl.when(holds)
    def _():
        near_copy().wait_send()

    @pl.when(away == 1)
    def _():
        given_copy.wait()
        out_ref[...] = taken[...]

    @pl.when(away == 0)
    def _():
        out_ref[...] = given[...]


def body(x_iterate, z_inverse, edge_src, edge_dst, edge_count):
    height, width = x_iterate.shape
    cells, _, slots = edge_src.shape
    hbm = pl.BlockSpec(memory_space=pltpu.HBM)
    values = pl.pallas_call(
        kernel,
        out_shape=jax.ShapeDtypeStruct((cells, 1, slots), jnp.float32),
        in_specs=[hbm] * 4,
        out_specs=pl.BlockSpec(memory_space=pltpu.VMEM),
        scratch_shapes=[
            pltpu.VMEM((height, width), jnp.float32),
            pltpu.VMEM((height, width), jnp.float32),
            pltpu.VMEM((3, cells, PIECES, width, width), jnp.bfloat16),
            pltpu.VMEM((2, cells, 1, slots), jnp.int32),
            pltpu.VMEM((2, 1, cells * slots), jnp.int32),
            pltpu.VMEM((3, cells, STEPS, 1, cells * slots), jnp.int32),
            pltpu.VMEM((2, cells, STEPS, slots, width), jnp.float32),
            pltpu.VMEM((2, cells, STEPS, slots, width), jnp.float32),
            pltpu.VMEM((width, width), jnp.float32),
            pltpu.VMEM((slots, width), jnp.float32),
            pltpu.VMEM((cells, 1, slots), jnp.float32),
            pltpu.VMEM((cells, 1, slots), jnp.float32),
            pltpu.SemaphoreType.DMA((4,)),
            pltpu.SemaphoreType.DMA((2, cells, STEPS)),
            pltpu.SemaphoreType.DMA((3, cells, STEPS)),
            pltpu.SemaphoreType.DMA((2, cells, STEPS)),
            pltpu.SemaphoreType.DMA((2, cells, STEPS)),
            pltpu.SemaphoreType.DMA((2,)),
            pltpu.SemaphoreType.DMA((1,)),
            pltpu.SemaphoreType.DMA((2,)),
        ],
        compiler_params=pltpu.CompilerParams(collective_id=0, has_side_effects=True, vmem_limit_bytes=10 * 2**20),
        name="schur_row",
    )(*(pltpu.with_memory_space_constraint(operand, pltpu.HBM) for operand in (x_iterate, z_inverse, edge_src, edge_dst)))
    live = lax.broadcasted_iota(jnp.int32, values.shape, 2) < edge_count[:, :, None]
    return jnp.where(live, values, jnp.zeros_like(values))


def solution(mesh):
    return jax.shard_map(
        body,
        mesh=mesh,
        in_specs=(
            P("row", "col"),
            P("row", "col"),
            P("row", "col", None),
            P("row", "col", None),
            P("row", "col"),
        ),
        out_specs=P("row", "col", None),
        check_vma=False,
    )
```

```python
import jax
import jax.numpy as jnp
from jax import lax
from jax.experimental import pallas as pl
from jax.experimental.pallas import tpu as pltpu
from jax.sharding import PartitionSpec as P

STEPS = 2
PIECES = 2
MESH = pl.DeviceIdType.MESH


def split_parts(value, parts_ref, *index):
    rest = value
    for piece in range(PIECES):
        part = rest.astype(jnp.bfloat16)
        parts_ref[(*index, piece)] = part
        if piece + 1 < PIECES:
            rest = rest - part.astype(jnp.float32)


def kernel(
    x_hbm, z_hbm, src_hbm, dst_hbm, out_ref,
    x_vmem, z_vmem, parts, index_in, index_out, wanted, rows_out, rows_in, held, near_out, given, taken,
    local_sem, index_send, index_recv, rows_send, rows_recv, push_sem, near_sem, given_sem,
):
    row, col = lax.axis_index("row"), lax.axis_index("col")
    n_row, n_col = lax.axis_size("row"), lax.axis_size("col")
    slots = src_hbm.shape[2]
    width = parts.shape[3]
    cells = 2
    src_copy = pltpu.make_async_copy(src_hbm, index_in.at[0], local_sem.at[2])
    dst_copy = pltpu.make_async_copy(dst_hbm, index_in.at[1], local_sem.at[3])
    x_copy = pltpu.make_async_copy(x_hbm, x_vmem, local_sem.at[0])
    z_copy = pltpu.make_async_copy(z_hbm, z_vmem, local_sem.at[1])
    src_copy.start()
    dst_copy.start()
    x_copy.start()
    z_copy.start()

    layer, chips = n_row // 2, n_col // 4
    twin = lax.rem(row + layer, n_row)

    def moved(reader_row, reader_col):
        diagonal = lax.rem(reader_row, layer) + lax.rem(reader_col, n_col // 2) // 2
        return jnp.where(diagonal >= chips - 1, 0, reader_col // (n_col // 2))

    def working(reader_row, reader_col):
        return lax.rem(reader_row + layer * moved(reader_row, reader_col), n_row)

    def pushed(reader_row, reader_col, q):
        x, y = lax.rem(reader_row, layer), lax.rem(reader_col, n_col // 2) // 2
        busy = jnp.logical_and((x + 1) // 2 == 1, reader_row != 1)
        return jnp.logical_and(jnp.logical_and(x + y < chips, jnp.logical_or(reader_col < n_col // 2, busy)), q == 1)

    core = lax.rem(col, 2)
    even = col - core
    for_row = working(row, col)
    gives_cell = 1 - core
    gives_to = lax.rem(col - cells * row - gives_cell - 1 + 2 * n_col, n_col)
    gives = pushed(row, gives_to, gives_cell)
    holds = pushed(for_row, even, core)
    giver = (for_row, lax.rem(even + cells * for_row + 1 + core, n_col))
    near = [pushed(row, even, c) for c in range(cells)]
    work_near = [pushed(for_row, even, c) for c in range(cells)]

    x_owner = [lax.rem(col + cells * row + u, n_col) for u in range(3)]
    x_reader = [lax.rem(col - cells * row - u + 2 * n_col, n_col) for u in range(3)]
    half = col // cells
    z_owner = [lax.rem(row + half + d, n_row) for d in range(2)]
    z_reader = [lax.rem(row - half - d + 2 * n_row, n_row) for d in range(2)]
    links = [((row, x_reader[u]), x_owner[u] == col) for u in range(3)]
    links += [((z_reader[d], col), z_owner[d] == row) for d in range(2)]
    barrier = pltpu.get_barrier_semaphore()
    for device in ((twin, col), (row, even + 1 - core), (twin, even + 1 - core)):
        pl.semaphore_signal(barrier, inc=1, device_id=device, device_id_type=MESH)

    @pl.when(holds)
    def _():
        pl.semaphore_signal(barrier, inc=1, device_id=giver, device_id_type=MESH)

    for reader, own in links:
        @pl.when(jnp.logical_not(own))
        def _():
            pl.semaphore_signal(barrier, inc=1, device_id=reader, device_id_type=MESH)

    src_copy.wait()
    dst_copy.wait()
    for which in range(2):
        index_out[which, :, :slots] = index_in[which, 0]
        index_out[which, :, slots:] = index_in[which, 1]
    pl.semaphore_wait(barrier, 3 + jnp.where(gives, 1, 0) + sum(jnp.where(own, 0, 1) for _, own in links))

    def from_near(c, s):
        return jnp.logical_and(near[c], core == 1 - s)

    def owner_of(kind, c, s):
        block = lax.rem(col + cells * row + c + s, n_col)
        if kind == 0:
            close = from_near(c, s)
            return jnp.where(close, for_row, row), jnp.where(close, even + c, block), jnp.where(close, 0, c), jnp.where(close, 2, 0)
        return block // cells, col, lax.rem(block, cells), 1

    def index_copy(kind, c, s):
        orow, ocol, p, to = owner_of(kind, c, s)
        return pltpu.make_async_remote_copy(
            src_ref=index_out.at[kind], dst_ref=wanted.at[to, p, s], send_sem=index_send.at[kind, c, s],
            recv_sem=index_recv.at[to, p, s], device_id=(orow, ocol), device_id_type=MESH)

    def owner_self(kind, c, s):
        orow, ocol, _, _ = owner_of(kind, c, s)
        return jnp.logical_and(orow == row, ocol == col)

    tasks = [(k, c, s) for k in (1, 0) for c in range(cells) for s in range(STEPS)]
    for t in tasks[cells * STEPS:] + tasks[:cells * STEPS]:
        @pl.when(jnp.logical_not(owner_self(*t)))
        def _(t=t):
            index_copy(*t).start()

        @pl.when(owner_self(*t))
        def _(t=t):
            _, _, p, to = owner_of(*t)
            wanted[to, p, t[2]] = index_out[t[0]]

    x_copy.wait()
    push_copy = pltpu.make_async_remote_copy(
        src_ref=x_vmem.at[pl.ds(pl.multiple_of(gives_cell * width, width), width)], dst_ref=held, send_sem=push_sem.at[0],
        recv_sem=push_sem.at[1], device_id=(working(row, gives_to), gives_to + gives_cell), device_id_type=MESH)

    @pl.when(gives)
    def _():
        push_copy.start()

    for c in range(cells):
        split_parts(x_vmem[c * width:(c + 1) * width, :], parts, 0, c)
    z_copy.wait()
    for b in range(cells):
        split_parts(jnp.transpose(z_vmem[b * width:(b + 1) * width, :]), parts, 1, b)

    def reader_of(kind, p, s):
        x_col = lax.rem(col - cells * row - p - s + 2 * n_col, n_col)
        block = lax.rem(cells * row + p - col - s + 2 * n_col, n_col)
        isz = kind == 1
        return jnp.where(isz, block // cells, row), jnp.where(isz, col, x_col), jnp.where(isz, lax.rem(block, cells), p)

    def rows_copy(kind, p, s):
        rrow, rcol, c = reader_of(kind, p, s)
        return pltpu.make_async_remote_copy(
            src_ref=rows_out.at[kind, p, s], dst_ref=rows_in.at[kind, c, s], send_sem=rows_send.at[kind, p, s],
            recv_sem=rows_recv.at[kind, c, s], device_id=(working(rrow, rcol), rcol), device_id_type=MESH)

    def stays(kind, p, s):
        rrow, rcol, c = reader_of(kind, p, s)
        return jnp.logical_and(working(rrow, rcol) == row, rcol == col)

    def handle(kind, p, s):
        rrow, rcol, c = reader_of(kind, p, s)

        @pl.when(jnp.logical_not(jnp.logical_and(rrow == row, rcol == col)))
        def _():
            pltpu.make_async_remote_copy(
                src_ref=index_out.at[0], dst_ref=wanted.at[kind, p, s], send_sem=index_send.at[kind, p, s],
                recv_sem=index_recv.at[kind, p, s], device_id=(row, col), device_id_type=MESH).wait_recv()

        rows_out[kind, p, s] = gathered(wanted[kind, p, s], c, kind, p)

        @pl.when(jnp.logical_not(stays(kind, p, s)))
        def _():
            rows_copy(kind, p, s).start()

    def gathered(both, c, kind, p):
        upper = jnp.broadcast_to(c, both.shape) == 1
        mine = jnp.where(upper, pltpu.roll(both, slots, 1), both)
        down = jnp.transpose(jnp.broadcast_to(mine, (2 * slots, 2 * slots)))[:slots]
        chosen = jnp.concatenate(
            [(down == lax.broadcasted_iota(jnp.int32, down.shape, 1) + first).astype(jnp.float32)
             for first in range(0, width, 2 * slots)], axis=1).astype(jnp.bfloat16)
        total = jnp.dot(chosen, parts[kind, p, 0], preferred_element_type=jnp.float32)
        for piece in range(1, PIECES):
            total += jnp.dot(chosen, parts[kind, p, piece], preferred_element_type=jnp.float32)
        return total

    def skips(kind, p):
        return jnp.logical_and(gives, gives_cell == p) if kind == 0 else row < 0

    for t in tasks:
        @pl.when(jnp.logical_not(skips(*t[:2])))
        def _(t=t):
            handle(*t)

    def near_copy():
        s = core
        return pltpu.make_async_remote_copy(
            src_ref=near_out, dst_ref=rows_in.at[0, core, s], send_sem=near_sem.at[0], recv_sem=rows_recv.at[0, core, s],
            device_id=(row, even + 1 - core), device_id_type=MESH)

    @pl.when(holds)
    def _():
        push_copy.wait_recv()
        split_parts(held[...], parts, 2, 0)
        pltpu.make_async_remote_copy(
            src_ref=index_out.at[0], dst_ref=wanted.at[2, 0, core], send_sem=index_send.at[0, 0, 0],
            recv_sem=index_recv.at[2, 0, core], device_id=(row, col), device_id_type=MESH).wait_recv()
        near_out[...] = gathered(wanted[2, 0, core], core, 2, 0)
        near_copy().start()

        @pl.when(for_row != row)
        def _():
            pltpu.make_async_remote_copy(
                src_ref=index_out.at[0], dst_ref=wanted.at[2, 0, 1 - core], send_sem=index_send.at[0, 0, 0],
                recv_sem=index_recv.at[2, 0, 1 - core], device_id=(row, col), device_id_type=MESH).wait_recv()

        rows_in[0, core, 1 - core] = gathered(wanted[2, 0, 1 - core], core, 2, 0)

    for t in tasks:
        @pl.when(jnp.logical_not(owner_self(*t)))
        def _(t=t):
            index_copy(*t).wait_send()

    for t in tasks[:cells * STEPS]:
        @pl.when(jnp.logical_not(jnp.logical_or(stays(*t), skips(*t[:2]))))
        def _(t=t):
            rows_copy(*t).wait_send()

    away = moved(row, col)
    for c in range(cells):
        total = None
        for s in range(STEPS):
            block = lax.rem(col + cells * for_row + c + s, n_col)
            close = jnp.logical_and(work_near[c], core == 1 - s)
            x_here = jnp.logical_and(jnp.logical_and(away == 0, block == col), jnp.logical_not(close))
            x_got = jnp.logical_or(x_here, jnp.logical_and(close, core == c))
            z_here = block // cells == row
            for kind, here in ((0, x_got), (1, z_here)):
                @pl.when(jnp.logical_not(here))
                def _(kind=kind, c=c, s=s):
                    pltpu.make_async_remote_copy(
                        src_ref=rows_out.at[kind, c, s], dst_ref=rows_in.at[kind, c, s], send_sem=rows_send.at[kind, c, s],
                        recv_sem=rows_recv.at[kind, c, s], device_id=(row, col), device_id_type=MESH).wait_recv()
            slot = lax.rem(block, cells)
            x_side = jnp.where(x_here, rows_out[0, c, s], rows_in[0, c, s])
            z_side = jnp.where(z_here, rows_out[1, slot, s], rows_in[1, c, s])
            term = x_side * z_side
            total = term if total is None else total + term
        folded = total[:, :slots]
        for at in range(slots, width, slots):
            folded = folded + total[:, at:at + slots]
        given[c] = jnp.sum(jnp.transpose(folded), axis=0, keepdims=True)

    given_copy = pltpu.make_async_remote_copy(
        src_ref=given, dst_ref=taken, send_sem=given_sem.at[0], recv_sem=given_sem.at[1],
        device_id=(twin, col), device_id_type=MESH)

    @pl.when(away == 1)
    def _():
        given_copy.start()

    for t in tasks[cells * STEPS:]:
        @pl.when(jnp.logical_not(jnp.logical_or(stays(*t), skips(*t[:2]))))
        def _(t=t):
            rows_copy(*t).wait_send()

    @pl.when(gives)
    def _():
        push_copy.wait_send()

    @pl.when(holds)
    def _():
        near_copy().wait_send()

    @pl.when(away == 1)
    def _():
        given_copy.wait()
        out_ref[...] = taken[...]

    @pl.when(away == 0)
    def _():
        out_ref[...] = given[...]


def body(x_iterate, z_inverse, edge_src, edge_dst, edge_count):
    height, width = x_iterate.shape
    cells, _, slots = edge_src.shape
    hbm = pl.BlockSpec(memory_space=pltpu.HBM)
    values = pl.pallas_call(
        kernel,
        out_shape=jax.ShapeDtypeStruct((cells, 1, slots), jnp.float32),
        in_specs=[hbm] * 4,
        out_specs=pl.BlockSpec(memory_space=pltpu.VMEM),
        scratch_shapes=[
            pltpu.VMEM((height, width), jnp.float32),
            pltpu.VMEM((height, width), jnp.float32),
            pltpu.VMEM((3, cells, PIECES, width, width), jnp.bfloat16),
            pltpu.VMEM((2, cells, 1, slots), jnp.int32),
            pltpu.VMEM((2, 1, cells * slots), jnp.int32),
            pltpu.VMEM((3, cells, STEPS, 1, cells * slots), jnp.int32),
            pltpu.VMEM((2, cells, STEPS, slots, width), jnp.float32),
            pltpu.VMEM((2, cells, STEPS, slots, width), jnp.float32),
            pltpu.VMEM((width, width), jnp.float32),
            pltpu.VMEM((slots, width), jnp.float32),
            pltpu.VMEM((cells, 1, slots), jnp.float32),
            pltpu.VMEM((cells, 1, slots), jnp.float32),
            pltpu.SemaphoreType.DMA((4,)),
            pltpu.SemaphoreType.DMA((2, cells, STEPS)),
            pltpu.SemaphoreType.DMA((3, cells, STEPS)),
            pltpu.SemaphoreType.DMA((2, cells, STEPS)),
            pltpu.SemaphoreType.DMA((2, cells, STEPS)),
            pltpu.SemaphoreType.DMA((2,)),
            pltpu.SemaphoreType.DMA((1,)),
            pltpu.SemaphoreType.DMA((2,)),
        ],
        compiler_params=pltpu.CompilerParams(collective_id=0, has_side_effects=True, vmem_limit_bytes=10 * 2**20),
        name="schur_row",
    )(*(pltpu.with_memory_space_constraint(operand, pltpu.HBM) for operand in (x_iterate, z_inverse, edge_src, edge_dst)))
    live = lax.broadcasted_iota(jnp.int32, values.shape, 2) < edge_count[:, :, None]
    return jnp.where(live, values, jnp.zeros_like(values))


def solution(mesh):
    return jax.shard_map(
        body,
        mesh=mesh,
        in_specs=(
            P("row", "col"),
            P("row", "col"),
            P("row", "col", None),
            P("row", "col", None),
            P("row", "col"),
        ),
        out_specs=P("row", "col", None),
        check_vma=False,
    )
```

```python
import jax
import jax.numpy as jnp
from jax import lax
from jax.experimental import pallas as pl
from jax.experimental.pallas import tpu as pltpu
from jax.sharding import PartitionSpec as P

STEPS = 2
PIECES = 2
MESH = pl.DeviceIdType.MESH


def split_parts(value, parts_ref, *index):
    rest = value
    for piece in range(PIECES):
        part = rest.astype(jnp.bfloat16)
        parts_ref[(*index, piece)] = part
        if piece + 1 < PIECES:
            rest = rest - part.astype(jnp.float32)


def kernel(
    x_hbm, z_hbm, src_hbm, dst_hbm, out_ref,
    x_vmem, z_vmem, parts, index_in, index_out, wanted, rows_out, rows_in, held, near_out, given, taken,
    local_sem, index_send, index_recv, rows_send, rows_recv, push_sem, near_sem, given_sem,
):
    row, col = lax.axis_index("row"), lax.axis_index("col")
    n_row, n_col = lax.axis_size("row"), lax.axis_size("col")
    slots = src_hbm.shape[2]
    width = parts.shape[3]
    cells = 2
    src_copy = pltpu.make_async_copy(src_hbm, index_in.at[0], local_sem.at[2])
    dst_copy = pltpu.make_async_copy(dst_hbm, index_in.at[1], local_sem.at[3])
    x_copy = pltpu.make_async_copy(x_hbm, x_vmem, local_sem.at[0])
    z_copy = pltpu.make_async_copy(z_hbm, z_vmem, local_sem.at[1])
    src_copy.start()
    dst_copy.start()
    x_copy.start()
    z_copy.start()

    layer, chips = n_row // 2, n_col // 4
    twin = lax.rem(row + layer, n_row)

    def moved(reader_row, reader_col):
        diagonal = lax.rem(reader_row, layer) + lax.rem(reader_col, n_col // 2) // 2
        return jnp.where(diagonal >= chips - 1, 0, reader_col // (n_col // 2))

    def working(reader_row, reader_col):
        return lax.rem(reader_row + layer * moved(reader_row, reader_col), n_row)

    def pushed(reader_row, reader_col, q):
        x, y = lax.rem(reader_row, layer), lax.rem(reader_col, n_col // 2) // 2
        busy = jnp.logical_and((x + 1) // 2 == 1, reader_row != 1)
        return jnp.logical_and(jnp.logical_and(x + y < chips, jnp.logical_or(reader_col < n_col // 2, busy)), q == 1)

    core = lax.rem(col, 2)
    even = col - core
    for_row = working(row, col)
    gives_cell = 1 - core
    gives_to = lax.rem(col - cells * row - gives_cell - 1 + 2 * n_col, n_col)
    gives = pushed(row, gives_to, gives_cell)
    holds = pushed(for_row, even, core)
    giver = (for_row, lax.rem(even + cells * for_row + 1 + core, n_col))
    near = [pushed(row, even, c) for c in range(cells)]
    work_near = [pushed(for_row, even, c) for c in range(cells)]

    x_owner = [lax.rem(col + cells * row + u, n_col) for u in range(3)]
    x_reader = [lax.rem(col - cells * row - u + 2 * n_col, n_col) for u in range(3)]
    half = col // cells
    z_owner = [lax.rem(row + half + d, n_row) for d in range(2)]
    z_reader = [lax.rem(row - half - d + 2 * n_row, n_row) for d in range(2)]
    links = [((row, x_reader[u]), x_owner[u] == col) for u in range(3)]
    links += [((z_reader[d], col), z_owner[d] == row) for d in range(2)]
    barrier = pltpu.get_barrier_semaphore()
    for device in ((twin, col), (row, even + 1 - core), (twin, even + 1 - core)):
        pl.semaphore_signal(barrier, inc=1, device_id=device, device_id_type=MESH)

    @pl.when(holds)
    def _():
        pl.semaphore_signal(barrier, inc=1, device_id=giver, device_id_type=MESH)

    for reader, own in links:
        @pl.when(jnp.logical_not(own))
        def _():
            pl.semaphore_signal(barrier, inc=1, device_id=reader, device_id_type=MESH)

    src_copy.wait()
    dst_copy.wait()
    for which in range(2):
        index_out[which, :, :slots] = index_in[which, 0]
        index_out[which, :, slots:] = index_in[which, 1]
    pl.semaphore_wait(barrier, 3 + jnp.where(gives, 1, 0) + sum(jnp.where(own, 0, 1) for _, own in links))

    messages = [
        (0, (row, x_owner[u]), u, x_owner[u] == col, jnp.logical_and(near[1], core == 0) if u == 2 else None) for u in range(3)
    ]
    messages += [(1, (z_owner[d], col), 3 + d, z_owner[d] == row, None) for d in range(2)]
    messages += [(0, (for_row, even + 1), 6 - core, jnp.logical_and(for_row == row, core == 1), jnp.logical_not(near[1]))]

    def index_copy(number):
        which, device, slot, _, _ = messages[number]
        return pltpu.make_async_remote_copy(
            src_ref=index_out.at[which], dst_ref=wanted.at[slot], send_sem=index_send.at[number],
            recv_sem=index_recv.at[slot], device_id=device, device_id_type=MESH)

    def leaves(number):
        _, _, _, own, dropped = messages[number]
        out = jnp.logical_not(own)
        return out if dropped is None else jnp.logical_and(out, jnp.logical_not(dropped))

    for number in (0, 1, 2, 5, 3, 4):
        @pl.when(leaves(number))
        def _(number=number):
            index_copy(number).start()

        which, _, slot, own, dropped = messages[number]

        @pl.when(own if dropped is None else jnp.logical_and(own, jnp.logical_not(dropped)))
        def _(which=which, slot=slot):
            wanted[slot] = index_out[which]

    def index_arrival(slot):
        return pltpu.make_async_remote_copy(
            src_ref=index_out.at[0], dst_ref=wanted.at[slot], send_sem=index_send.at[0],
            recv_sem=index_recv.at[slot], device_id=(row, col), device_id_type=MESH)

    tasks = [(k, c, s) for k in (1, 0) for c in range(cells) for s in range(STEPS)]
    x_copy.wait()
    push_copy = pltpu.make_async_remote_copy(
        src_ref=x_vmem.at[pl.ds(pl.multiple_of(gives_cell * width, width), width)], dst_ref=held, send_sem=push_sem.at[0],
        recv_sem=push_sem.at[1], device_id=(working(row, gives_to), gives_to + gives_cell), device_id_type=MESH)

    @pl.when(gives)
    def _():
        push_copy.start()

    for c in range(cells):
        split_parts(x_vmem[c * width:(c + 1) * width, :], parts, 0, c)
    z_copy.wait()
    for b in range(cells):
        split_parts(jnp.transpose(z_vmem[b * width:(b + 1) * width, :]), parts, 1, b)

    def reader_of(kind, p, s):
        x_col = lax.rem(col - cells * row - p - s + 2 * n_col, n_col)
        block = lax.rem(cells * row + p - col - s + 2 * n_col, n_col)
        isz = kind == 1
        return jnp.where(isz, block // cells, row), jnp.where(isz, col, x_col), jnp.where(isz, lax.rem(block, cells), p)

    def rows_copy(kind, p, s):
        rrow, rcol, c = reader_of(kind, p, s)
        return pltpu.make_async_remote_copy(
            src_ref=rows_out.at[kind, p, s], dst_ref=rows_in.at[kind, c, s], send_sem=rows_send.at[kind, p, s],
            recv_sem=rows_recv.at[kind, c, s], device_id=(working(rrow, rcol), rcol), device_id_type=MESH)

    def stays(kind, p, s):
        rrow, rcol, c = reader_of(kind, p, s)
        return jnp.logical_and(working(rrow, rcol) == row, rcol == col)

    def handle(kind, p, s):
        rrow, rcol, c = reader_of(kind, p, s)
        slot = p + s if kind == 0 else 3 + (core + c + s) // 2
        arrives = jnp.logical_not(jnp.logical_and(rrow == row, rcol == col))
        if kind == 1 and p != s:
            arrives = jnp.logical_and(arrives, core == p)
        if (kind, p, s) != (0, 1, 0) and (kind, p, s) != (1, 1, 1):
            @pl.when(arrives)
            def _():
                index_arrival(slot).wait_recv()

        rows_out[kind, p, s] = gathered(wanted[slot], c, kind, p)

        @pl.when(jnp.logical_not(stays(kind, p, s)))
        def _():
            rows_copy(kind, p, s).start()

    def gathered(both, c, kind, p):
        upper = jnp.broadcast_to(c, both.shape) == 1
        mine = jnp.where(upper, pltpu.roll(both, slots, 1), both)
        down = jnp.transpose(jnp.broadcast_to(mine, (2 * slots, 2 * slots)))[:slots]
        chosen = jnp.concatenate(
            [(down == lax.broadcasted_iota(jnp.int32, down.shape, 1) + first).astype(jnp.float32)
             for first in range(0, width, 2 * slots)], axis=1).astype(jnp.bfloat16)
        total = jnp.dot(chosen, parts[kind, p, 0], preferred_element_type=jnp.float32)
        for piece in range(1, PIECES):
            total += jnp.dot(chosen, parts[kind, p, piece], preferred_element_type=jnp.float32)
        return total

    def skips(kind, p):
        return jnp.logical_and(gives, gives_cell == p) if kind == 0 else row < 0

    for t in tasks:
        @pl.when(jnp.logical_not(skips(*t[:2])))
        def _(t=t):
            handle(*t)

    def near_copy():
        s = core
        return pltpu.make_async_remote_copy(
            src_ref=near_out, dst_ref=rows_in.at[0, core, s], send_sem=near_sem.at[0], recv_sem=rows_recv.at[0, core, s],
            device_id=(row, even + 1 - core), device_id_type=MESH)

    @pl.when(holds)
    def _():
        push_copy.wait_recv()
        split_parts(held[...], parts, 2, 0)
        index_arrival(5 + core).wait_recv()
        near_out[...] = gathered(wanted[5 + core], core, 2, 0)
        near_copy().start()

        @pl.when(for_row != row)
        def _():
            index_arrival(6 - core).wait_recv()

        rows_in[0, core, 1 - core] = gathered(wanted[6 - core], core, 2, 0)

    for number in range(len(messages)):
        @pl.when(leaves(number))
        def _(number=number):
            index_copy(number).wait_send()

    for t in tasks[:cells * STEPS]:
        @pl.when(jnp.logical_not(jnp.logical_or(stays(*t), skips(*t[:2]))))
        def _(t=t):
            rows_copy(*t).wait_send()

    away = moved(row, col)
    for c in range(cells):
        total = None
        for s in range(STEPS):
            block = lax.rem(col + cells * for_row + c + s, n_col)
            close = jnp.logical_and(work_near[c], core == 1 - s)
            x_here = jnp.logical_and(jnp.logical_and(away == 0, block == col), jnp.logical_not(close))
            x_got = jnp.logical_or(x_here, jnp.logical_and(close, core == c))
            z_here = block // cells == row
            for kind, here in ((0, x_got), (1, z_here)):
                @pl.when(jnp.logical_not(here))
                def _(kind=kind, c=c, s=s):
                    pltpu.make_async_remote_copy(
                        src_ref=rows_out.at[kind, c, s], dst_ref=rows_in.at[kind, c, s], send_sem=rows_send.at[kind, c, s],
                        recv_sem=rows_recv.at[kind, c, s], device_id=(row, col), device_id_type=MESH).wait_recv()
            slot = lax.rem(block, cells)
            x_side = jnp.where(x_here, rows_out[0, c, s], rows_in[0, c, s])
            z_side = jnp.where(z_here, rows_out[1, slot, s], rows_in[1, c, s])
            term = x_side * z_side
            total = term if total is None else total + term
        folded = total[:, :slots]
        for at in range(slots, width, slots):
            folded = folded + total[:, at:at + slots]
        given[c] = jnp.sum(jnp.transpose(folded), axis=0, keepdims=True)

    given_copy = pltpu.make_async_remote_copy(
        src_ref=given, dst_ref=taken, send_sem=given_sem.at[0], recv_sem=given_sem.at[1],
        device_id=(twin, col), device_id_type=MESH)

    @pl.when(away == 1)
    def _():
        given_copy.start()

    for t in tasks[cells * STEPS:]:
        @pl.when(jnp.logical_not(jnp.logical_or(stays(*t), skips(*t[:2]))))
        def _(t=t):
            rows_copy(*t).wait_send()

    @pl.when(gives)
    def _():
        push_copy.wait_send()

    @pl.when(holds)
    def _():
        near_copy().wait_send()

    @pl.when(away == 1)
    def _():
        given_copy.wait()
        out_ref[...] = taken[...]

    @pl.when(away == 0)
    def _():
        out_ref[...] = given[...]


def body(x_iterate, z_inverse, edge_src, edge_dst, edge_count):
    height, width = x_iterate.shape
    cells, _, slots = edge_src.shape
    hbm = pl.BlockSpec(memory_space=pltpu.HBM)
    values = pl.pallas_call(
        kernel,
        out_shape=jax.ShapeDtypeStruct((cells, 1, slots), jnp.float32),
        in_specs=[hbm] * 4,
        out_specs=pl.BlockSpec(memory_space=pltpu.VMEM),
        scratch_shapes=[
            pltpu.VMEM((height, width), jnp.float32),
            pltpu.VMEM((height, width), jnp.float32),
            pltpu.VMEM((3, cells, PIECES, width, width), jnp.bfloat16),
            pltpu.VMEM((2, cells, 1, slots), jnp.int32),
            pltpu.VMEM((2, 1, cells * slots), jnp.int32),
            pltpu.VMEM((7, 1, cells * slots), jnp.int32),
            pltpu.VMEM((2, cells, STEPS, slots, width), jnp.float32),
            pltpu.VMEM((2, cells, STEPS, slots, width), jnp.float32),
            pltpu.VMEM((width, width), jnp.float32),
            pltpu.VMEM((slots, width), jnp.float32),
            pltpu.VMEM((cells, 1, slots), jnp.float32),
            pltpu.VMEM((cells, 1, slots), jnp.float32),
            pltpu.SemaphoreType.DMA((4,)),
            pltpu.SemaphoreType.DMA((6,)),
            pltpu.SemaphoreType.DMA((7,)),
            pltpu.SemaphoreType.DMA((2, cells, STEPS)),
            pltpu.SemaphoreType.DMA((2, cells, STEPS)),
            pltpu.SemaphoreType.DMA((2,)),
            pltpu.SemaphoreType.DMA((1,)),
            pltpu.SemaphoreType.DMA((2,)),
        ],
        compiler_params=pltpu.CompilerParams(collective_id=0, has_side_effects=True, vmem_limit_bytes=10 * 2**20),
        name="schur_row",
    )(*(pltpu.with_memory_space_constraint(operand, pltpu.HBM) for operand in (x_iterate, z_inverse, edge_src, edge_dst)))
    live = lax.broadcasted_iota(jnp.int32, values.shape, 2) < edge_count[:, :, None]
    return jnp.where(live, values, jnp.zeros_like(values))


def solution(mesh):
    return jax.shard_map(
        body,
        mesh=mesh,
        in_specs=(
            P("row", "col"),
            P("row", "col"),
            P("row", "col", None),
            P("row", "col", None),
            P("row", "col"),
        ),
        out_specs=P("row", "col", None),
        check_vma=False,
    )
```

```python
import jax
import jax.numpy as jnp
from jax import lax
from jax.experimental import pallas as pl
from jax.experimental.pallas import tpu as pltpu
from jax.sharding import PartitionSpec as P

STEPS = 2
PIECES = 2
MESH = pl.DeviceIdType.MESH


def split_parts(value, parts_ref, *index):
    rest = value
    for piece in range(PIECES):
        part = rest.astype(jnp.bfloat16)
        parts_ref[(*index, piece)] = part
        if piece + 1 < PIECES:
            rest = rest - part.astype(jnp.float32)


def kernel(
    x_hbm, z_hbm, src_hbm, dst_hbm, out_ref,
    x_vmem, z_vmem, parts, index_in, index_out, wanted, rows_out, rows_in, held, near_out, given, taken,
    local_sem, index_send, index_recv, rows_send, rows_recv, push_sem, near_sem, given_sem,
):
    row, col = lax.axis_index("row"), lax.axis_index("col")
    n_row, n_col = lax.axis_size("row"), lax.axis_size("col")
    slots = src_hbm.shape[2]
    width = parts.shape[3]
    cells = 2
    src_copy = pltpu.make_async_copy(src_hbm, index_in.at[0], local_sem.at[2])
    dst_copy = pltpu.make_async_copy(dst_hbm, index_in.at[1], local_sem.at[3])
    x_copy = pltpu.make_async_copy(x_hbm, x_vmem, local_sem.at[0])
    z_copy = pltpu.make_async_copy(z_hbm, z_vmem, local_sem.at[1])
    src_copy.start()
    dst_copy.start()
    x_copy.start()
    z_copy.start()

    layer, chips = n_row // 2, n_col // 4
    twin = lax.rem(row + layer, n_row)

    def moved(reader_row, reader_col):
        diagonal = lax.rem(reader_row, layer) + lax.rem(reader_col, n_col // 2) // 2
        return jnp.where(diagonal >= chips - 1, 0, reader_col // (n_col // 2))

    def working(reader_row, reader_col):
        return lax.rem(reader_row + layer * moved(reader_row, reader_col), n_row)

    def pushed(reader_row, reader_col, q):
        x, y = lax.rem(reader_row, layer), lax.rem(reader_col, n_col // 2) // 2
        busy = jnp.logical_and((x + 1) // 2 == 1, reader_row != 1)
        return jnp.logical_and(jnp.logical_or(jnp.logical_and(x + y < chips, jnp.logical_or(reader_col < n_col // 2, busy)), jnp.logical_and(x + y < chips - 1, x == 0)), q == 1)

    core = lax.rem(col, 2)
    even = col - core
    for_row = working(row, col)
    gives_cell = 1 - core
    gives_to = lax.rem(col - cells * row - gives_cell - 1 + 2 * n_col, n_col)
    gives = pushed(row, gives_to, gives_cell)
    holds = pushed(for_row, even, core)
    giver = (for_row, lax.rem(even + cells * for_row + 1 + core, n_col))
    near = [pushed(row, even, c) for c in range(cells)]
    work_near = [pushed(for_row, even, c) for c in range(cells)]

    x_owner = [lax.rem(col + cells * row + u, n_col) for u in range(3)]
    x_reader = [lax.rem(col - cells * row - u + 2 * n_col, n_col) for u in range(3)]
    half = col // cells
    z_owner = [lax.rem(row + half + d, n_row) for d in range(2)]
    z_reader = [lax.rem(row - half - d + 2 * n_row, n_row) for d in range(2)]
    links = [((row, x_reader[u]), x_owner[u] == col) for u in range(3)]
    links += [((z_reader[d], col), z_owner[d] == row) for d in range(2)]
    barrier = pltpu.get_barrier_semaphore()
    for device in ((twin, col), (row, even + 1 - core), (twin, even + 1 - core)):
        pl.semaphore_signal(barrier, inc=1, device_id=device, device_id_type=MESH)

    @pl.when(holds)
    def _():
        pl.semaphore_signal(barrier, inc=1, device_id=giver, device_id_type=MESH)

    for reader, own in links:
        @pl.when(jnp.logical_not(own))
        def _():
            pl.semaphore_signal(barrier, inc=1, device_id=reader, device_id_type=MESH)

    src_copy.wait()
    dst_copy.wait()
    for which in range(2):
        index_out[which, :, :slots] = index_in[which, 0]
        index_out[which, :, slots:] = index_in[which, 1]
    pl.semaphore_wait(barrier, 3 + jnp.where(gives, 1, 0) + sum(jnp.where(own, 0, 1) for _, own in links))

    messages = [
        (0, (row, x_owner[u]), u, x_owner[u] == col, jnp.logical_and(near[1], core == 0) if u == 2 else None) for u in range(3)
    ]
    messages += [(1, (z_owner[d], col), 3 + d, z_owner[d] == row, None) for d in range(2)]
    messages += [(0, (for_row, even + 1), 6 - core, jnp.logical_and(for_row == row, core == 1), jnp.logical_not(near[1]))]

    def index_copy(number):
        which, device, slot, _, _ = messages[number]
        return pltpu.make_async_remote_copy(
            src_ref=index_out.at[which], dst_ref=wanted.at[slot], send_sem=index_send.at[number],
            recv_sem=index_recv.at[slot], device_id=device, device_id_type=MESH)

    def leaves(number):
        _, _, _, own, dropped = messages[number]
        out = jnp.logical_not(own)
        return out if dropped is None else jnp.logical_and(out, jnp.logical_not(dropped))

    for number in (0, 1, 2, 5, 3, 4):
        @pl.when(leaves(number))
        def _(number=number):
            index_copy(number).start()

        which, _, slot, own, dropped = messages[number]

        @pl.when(own if dropped is None else jnp.logical_and(own, jnp.logical_not(dropped)))
        def _(which=which, slot=slot):
            wanted[slot] = index_out[which]

    def index_arrival(slot):
        return pltpu.make_async_remote_copy(
            src_ref=index_out.at[0], dst_ref=wanted.at[slot], send_sem=index_send.at[0],
            recv_sem=index_recv.at[slot], device_id=(row, col), device_id_type=MESH)

    tasks = [(k, c, s) for k in (1, 0) for c in range(cells) for s in range(STEPS)]
    x_copy.wait()
    push_copy = pltpu.make_async_remote_copy(
        src_ref=x_vmem.at[pl.ds(pl.multiple_of(gives_cell * width, width), width)], dst_ref=held, send_sem=push_sem.at[0],
        recv_sem=push_sem.at[1], device_id=(working(row, gives_to), gives_to + gives_cell), device_id_type=MESH)

    @pl.when(gives)
    def _():
        push_copy.start()

    for c in range(cells):
        split_parts(x_vmem[c * width:(c + 1) * width, :], parts, 0, c)
    z_copy.wait()
    for b in range(cells):
        split_parts(jnp.transpose(z_vmem[b * width:(b + 1) * width, :]), parts, 1, b)

    def reader_of(kind, p, s):
        x_col = lax.rem(col - cells * row - p - s + 2 * n_col, n_col)
        block = lax.rem(cells * row + p - col - s + 2 * n_col, n_col)
        isz = kind == 1
        return jnp.where(isz, block // cells, row), jnp.where(isz, col, x_col), jnp.where(isz, lax.rem(block, cells), p)

    def rows_copy(kind, p, s):
        rrow, rcol, c = reader_of(kind, p, s)
        return pltpu.make_async_remote_copy(
            src_ref=rows_out.at[kind, p, s], dst_ref=rows_in.at[kind, c, s], send_sem=rows_send.at[kind, p, s],
            recv_sem=rows_recv.at[kind, c, s], device_id=(working(rrow, rcol), rcol), device_id_type=MESH)

    def stays(kind, p, s):
        rrow, rcol, c = reader_of(kind, p, s)
        return jnp.logical_and(working(rrow, rcol) == row, rcol == col)

    def handle(kind, p, s):
        rrow, rcol, c = reader_of(kind, p, s)
        slot = p + s if kind == 0 else 3 + (core + c + s) // 2
        arrives = jnp.logical_not(jnp.logical_and(rrow == row, rcol == col))
        if kind == 1 and p != s:
            arrives = jnp.logical_and(arrives, core == p)
        if (kind, p, s) != (0, 1, 0) and (kind, p, s) != (1, 1, 1):
            @pl.when(arrives)
            def _():
                index_arrival(slot).wait_recv()

        rows_out[kind, p, s] = gathered(wanted[slot], c, kind, p)

        @pl.when(jnp.logical_not(stays(kind, p, s)))
        def _():
            rows_copy(kind, p, s).start()

    def gathered(both, c, kind, p):
        upper = jnp.broadcast_to(c, both.shape) == 1
        mine = jnp.where(upper, pltpu.roll(both, slots, 1), both)
        down = jnp.transpose(jnp.broadcast_to(mine, (2 * slots, 2 * slots)))[:slots]
        chosen = jnp.concatenate(
            [(down == lax.broadcasted_iota(jnp.int32, down.shape, 1) + first).astype(jnp.float32)
             for first in range(0, width, 2 * slots)], axis=1).astype(jnp.bfloat16)
        total = jnp.dot(chosen, parts[kind, p, 0], preferred_element_type=jnp.float32)
        for piece in range(1, PIECES):
            total += jnp.dot(chosen, parts[kind, p, piece], preferred_element_type=jnp.float32)
        return total

    def skips(kind, p):
        return jnp.logical_and(gives, gives_cell == p) if kind == 0 else row < 0

    for t in tasks:
        @pl.when(jnp.logical_not(skips(*t[:2])))
        def _(t=t):
            handle(*t)

    def near_copy():
        s = core
        return pltpu.make_async_remote_copy(
            src_ref=near_out, dst_ref=rows_in.at[0, core, s], send_sem=near_sem.at[0], recv_sem=rows_recv.at[0, core, s],
            device_id=(row, even + 1 - core), device_id_type=MESH)

    @pl.when(holds)
    def _():
        push_copy.wait_recv()
        split_parts(held[...], parts, 2, 0)
        index_arrival(5 + core).wait_recv()
        near_out[...] = gathered(wanted[5 + core], core, 2, 0)
        near_copy().start()

        @pl.when(for_row != row)
        def _():
            index_arrival(6 - core).wait_recv()

        rows_in[0, core, 1 - core] = gathered(wanted[6 - core], core, 2, 0)

    for number in range(len(messages)):
        @pl.when(leaves(number))
        def _(number=number):
            index_copy(number).wait_send()

    for t in tasks[:cells * STEPS]:
        @pl.when(jnp.logical_not(jnp.logical_or(stays(*t), skips(*t[:2]))))
        def _(t=t):
            rows_copy(*t).wait_send()

    away = moved(row, col)
    for c in range(cells):
        total = None
        for s in range(STEPS):
            block = lax.rem(col + cells * for_row + c + s, n_col)
            close = jnp.logical_and(work_near[c], core == 1 - s)
            x_here = jnp.logical_and(jnp.logical_and(away == 0, block == col), jnp.logical_not(close))
            x_got = jnp.logical_or(x_here, jnp.logical_and(close, core == c))
            z_here = block // cells == row
            for kind, here in ((0, x_got), (1, z_here)):
                @pl.when(jnp.logical_not(here))
                def _(kind=kind, c=c, s=s):
                    pltpu.make_async_remote_copy(
                        src_ref=rows_out.at[kind, c, s], dst_ref=rows_in.at[kind, c, s], send_sem=rows_send.at[kind, c, s],
                        recv_sem=rows_recv.at[kind, c, s], device_id=(row, col), device_id_type=MESH).wait_recv()
            slot = lax.rem(block, cells)
            x_side = jnp.where(x_here, rows_out[0, c, s], rows_in[0, c, s])
            z_side = jnp.where(z_here, rows_out[1, slot, s], rows_in[1, c, s])
            term = x_side * z_side
            total = term if total is None else total + term
        folded = total[:, :slots]
        for at in range(slots, width, slots):
            folded = folded + total[:, at:at + slots]
        given[c] = jnp.sum(jnp.transpose(folded), axis=0, keepdims=True)

    given_copy = pltpu.make_async_remote_copy(
        src_ref=given, dst_ref=taken, send_sem=given_sem.at[0], recv_sem=given_sem.at[1],
        device_id=(twin, col), device_id_type=MESH)

    @pl.when(away == 1)
    def _():
        given_copy.start()

    for t in tasks[cells * STEPS:]:
        @pl.when(jnp.logical_not(jnp.logical_or(stays(*t), skips(*t[:2]))))
        def _(t=t):
            rows_copy(*t).wait_send()

    @pl.when(gives)
    def _():
        push_copy.wait_send()

    @pl.when(holds)
    def _():
        near_copy().wait_send()

    @pl.when(away == 1)
    def _():
        given_copy.wait()
        out_ref[...] = taken[...]

    @pl.when(away == 0)
    def _():
        out_ref[...] = given[...]


def body(x_iterate, z_inverse, edge_src, edge_dst, edge_count):
    height, width = x_iterate.shape
    cells, _, slots = edge_src.shape
    hbm = pl.BlockSpec(memory_space=pltpu.HBM)
    values = pl.pallas_call(
        kernel,
        out_shape=jax.ShapeDtypeStruct((cells, 1, slots), jnp.float32),
        in_specs=[hbm] * 4,
        out_specs=pl.BlockSpec(memory_space=pltpu.VMEM),
        scratch_shapes=[
            pltpu.VMEM((height, width), jnp.float32),
            pltpu.VMEM((height, width), jnp.float32),
            pltpu.VMEM((3, cells, PIECES, width, width), jnp.bfloat16),
            pltpu.VMEM((2, cells, 1, slots), jnp.int32),
            pltpu.VMEM((2, 1, cells * slots), jnp.int32),
            pltpu.VMEM((7, 1, cells * slots), jnp.int32),
            pltpu.VMEM((2, cells, STEPS, slots, width), jnp.float32),
            pltpu.VMEM((2, cells, STEPS, slots, width), jnp.float32),
            pltpu.VMEM((width, width), jnp.float32),
            pltpu.VMEM((slots, width), jnp.float32),
            pltpu.VMEM((cells, 1, slots), jnp.float32),
            pltpu.VMEM((cells, 1, slots), jnp.float32),
            pltpu.SemaphoreType.DMA((4,)),
            pltpu.SemaphoreType.DMA((6,)),
            pltpu.SemaphoreType.DMA((7,)),
            pltpu.SemaphoreType.DMA((2, cells, STEPS)),
            pltpu.SemaphoreType.DMA((2, cells, STEPS)),
            pltpu.SemaphoreType.DMA((2,)),
            pltpu.SemaphoreType.DMA((1,)),
            pltpu.SemaphoreType.DMA((2,)),
        ],
        compiler_params=pltpu.CompilerParams(collective_id=0, has_side_effects=True, vmem_limit_bytes=10 * 2**20),
        name="schur_row",
    )(*(pltpu.with_memory_space_constraint(operand, pltpu.HBM) for operand in (x_iterate, z_inverse, edge_src, edge_dst)))
    live = lax.broadcasted_iota(jnp.int32, values.shape, 2) < edge_count[:, :, None]
    return jnp.where(live, values, jnp.zeros_like(values))


def solution(mesh):
    return jax.shard_map(
        body,
        mesh=mesh,
        in_specs=(
            P("row", "col"),
            P("row", "col"),
            P("row", "col", None),
            P("row", "col", None),
            P("row", "col"),
        ),
        out_specs=P("row", "col", None),
        check_vma=False,
    )
```

```python
import jax
import jax.numpy as jnp
from jax import lax
from jax.experimental import pallas as pl
from jax.experimental.pallas import tpu as pltpu
from jax.sharding import PartitionSpec as P

STEPS = 2
PIECES = 2
MESH = pl.DeviceIdType.MESH


def split_parts(value, parts_ref, *index):
    rest = value
    for piece in range(PIECES):
        part = rest.astype(jnp.bfloat16)
        parts_ref[(*index, piece)] = part
        if piece + 1 < PIECES:
            rest = rest - part.astype(jnp.float32)


def kernel(
    x_hbm, z_hbm, src_hbm, dst_hbm, out_ref,
    x_vmem, z_vmem, parts, index_in, index_out, wanted, rows_out, rows_in, held, near_out, given, taken,
    local_sem, index_send, index_recv, rows_send, rows_recv, push_sem, near_sem, given_sem,
):
    row, col = lax.axis_index("row"), lax.axis_index("col")
    n_row, n_col = lax.axis_size("row"), lax.axis_size("col")
    slots = src_hbm.shape[2]
    width = parts.shape[3]
    cells = 2
    src_copy = pltpu.make_async_copy(src_hbm, index_in.at[0], local_sem.at[2])
    dst_copy = pltpu.make_async_copy(dst_hbm, index_in.at[1], local_sem.at[3])
    x_copy = pltpu.make_async_copy(x_hbm, x_vmem, local_sem.at[0])
    z_copy = pltpu.make_async_copy(z_hbm, z_vmem, local_sem.at[1])
    src_copy.start()
    dst_copy.start()
    x_copy.start()
    z_copy.start()

    layer, chips = n_row // 2, n_col // 4
    twin = lax.rem(row + layer, n_row)

    def moved(reader_row, reader_col):
        diagonal = lax.rem(reader_row, layer) + lax.rem(reader_col, n_col // 2) // 2
        return jnp.where(diagonal >= chips - 1, 0, reader_col // (n_col // 2))

    def working(reader_row, reader_col):
        return lax.rem(reader_row + layer * moved(reader_row, reader_col), n_row)

    def pushed(reader_row, reader_col, q):
        x, y = lax.rem(reader_row, layer), lax.rem(reader_col, n_col // 2) // 2
        busy = jnp.logical_and((x + 1) // 2 == 1, reader_row != 1)
        return jnp.logical_and(jnp.logical_or(jnp.logical_and(x + y < chips, jnp.logical_or(reader_col < n_col // 2, busy)), jnp.logical_and(x + y < chips, lax.rem(x, 3) == 0)), q == 1)

    core = lax.rem(col, 2)
    even = col - core
    for_row = working(row, col)
    gives_cell = 1 - core
    gives_to = lax.rem(col - cells * row - gives_cell - 1 + 2 * n_col, n_col)
    gives = pushed(row, gives_to, gives_cell)
    holds = pushed(for_row, even, core)
    giver = (for_row, lax.rem(even + cells * for_row + 1 + core, n_col))
    near = [pushed(row, even, c) for c in range(cells)]
    work_near = [pushed(for_row, even, c) for c in range(cells)]

    x_owner = [lax.rem(col + cells * row + u, n_col) for u in range(3)]
    x_reader = [lax.rem(col - cells * row - u + 2 * n_col, n_col) for u in range(3)]
    half = col // cells
    z_owner = [lax.rem(row + half + d, n_row) for d in range(2)]
    z_reader = [lax.rem(row - half - d + 2 * n_row, n_row) for d in range(2)]
    links = [((row, x_reader[u]), x_owner[u] == col) for u in range(3)]
    links += [((z_reader[d], col), z_owner[d] == row) for d in range(2)]
    barrier = pltpu.get_barrier_semaphore()
    for device in ((twin, col), (row, even + 1 - core), (twin, even + 1 - core)):
        pl.semaphore_signal(barrier, inc=1, device_id=device, device_id_type=MESH)

    @pl.when(holds)
    def _():
        pl.semaphore_signal(barrier, inc=1, device_id=giver, device_id_type=MESH)

    for reader, own in links:
        @pl.when(jnp.logical_not(own))
        def _():
            pl.semaphore_signal(barrier, inc=1, device_id=reader, device_id_type=MESH)

    src_copy.wait()
    dst_copy.wait()
    for which in range(2):
        index_out[which, :, :slots] = index_in[which, 0]
        index_out[which, :, slots:] = index_in[which, 1]
    pl.semaphore_wait(barrier, 3 + jnp.where(gives, 1, 0) + sum(jnp.where(own, 0, 1) for _, own in links))

    messages = [
        (0, (row, x_owner[u]), u, x_owner[u] == col, jnp.logical_and(near[1], core == 0) if u == 2 else None) for u in range(3)
    ]
    messages += [(1, (z_owner[d], col), 3 + d, z_owner[d] == row, None) for d in range(2)]
    messages += [(0, (for_row, even + 1), 6 - core, jnp.logical_and(for_row == row, core == 1), jnp.logical_not(near[1]))]

    def index_copy(number):
        which, device, slot, _, _ = messages[number]
        return pltpu.make_async_remote_copy(
            src_ref=index_out.at[which], dst_ref=wanted.at[slot], send_sem=index_send.at[number],
            recv_sem=index_recv.at[slot], device_id=device, device_id_type=MESH)

    def leaves(number):
        _, _, _, own, dropped = messages[number]
        out = jnp.logical_not(own)
        return out if dropped is None else jnp.logical_and(out, jnp.logical_not(dropped))

    for number in (0, 1, 2, 5, 3, 4):
        @pl.when(leaves(number))
        def _(number=number):
            index_copy(number).start()

        which, _, slot, own, dropped = messages[number]

        @pl.when(own if dropped is None else jnp.logical_and(own, jnp.logical_not(dropped)))
        def _(which=which, slot=slot):
            wanted[slot] = index_out[which]

    def index_arrival(slot):
        return pltpu.make_async_remote_copy(
            src_ref=index_out.at[0], dst_ref=wanted.at[slot], send_sem=index_send.at[0],
            recv_sem=index_recv.at[slot], device_id=(row, col), device_id_type=MESH)

    tasks = [(k, c, s) for k in (1, 0) for c in range(cells) for s in range(STEPS)]
    x_copy.wait()
    push_copy = pltpu.make_async_remote_copy(
        src_ref=x_vmem.at[pl.ds(pl.multiple_of(gives_cell * width, width), width)], dst_ref=held, send_sem=push_sem.at[0],
        recv_sem=push_sem.at[1], device_id=(working(row, gives_to), gives_to + gives_cell), device_id_type=MESH)

    @pl.when(gives)
    def _():
        push_copy.start()

    for c in range(cells):
        split_parts(x_vmem[c * width:(c + 1) * width, :], parts, 0, c)
    z_copy.wait()
    for b in range(cells):
        split_parts(jnp.transpose(z_vmem[b * width:(b + 1) * width, :]), parts, 1, b)

    def reader_of(kind, p, s):
        x_col = lax.rem(col - cells * row - p - s + 2 * n_col, n_col)
        block = lax.rem(cells * row + p - col - s + 2 * n_col, n_col)
        isz = kind == 1
        return jnp.where(isz, block // cells, row), jnp.where(isz, col, x_col), jnp.where(isz, lax.rem(block, cells), p)

    def rows_copy(kind, p, s):
        rrow, rcol, c = reader_of(kind, p, s)
        return pltpu.make_async_remote_copy(
            src_ref=rows_out.at[kind, p, s], dst_ref=rows_in.at[kind, c, s], send_sem=rows_send.at[kind, p, s],
            recv_sem=rows_recv.at[kind, c, s], device_id=(working(rrow, rcol), rcol), device_id_type=MESH)

    def stays(kind, p, s):
        rrow, rcol, c = reader_of(kind, p, s)
        return jnp.logical_and(working(rrow, rcol) == row, rcol == col)

    def handle(kind, p, s):
        rrow, rcol, c = reader_of(kind, p, s)
        slot = p + s if kind == 0 else 3 + (core + c + s) // 2
        arrives = jnp.logical_not(jnp.logical_and(rrow == row, rcol == col))
        if kind == 1 and p != s:
            arrives = jnp.logical_and(arrives, core == p)
        if (kind, p, s) != (0, 1, 0) and (kind, p, s) != (1, 1, 1):
            @pl.when(arrives)
            def _():
                index_arrival(slot).wait_recv()

        rows_out[kind, p, s] = gathered(wanted[slot], c, kind, p)

        @pl.when(jnp.logical_not(stays(kind, p, s)))
        def _():
            rows_copy(kind, p, s).start()

    def gathered(both, c, kind, p):
        upper = jnp.broadcast_to(c, both.shape) == 1
        mine = jnp.where(upper, pltpu.roll(both, slots, 1), both)
        down = jnp.transpose(jnp.broadcast_to(mine, (2 * slots, 2 * slots)))[:slots]
        chosen = jnp.concatenate(
            [(down == lax.broadcasted_iota(jnp.int32, down.shape, 1) + first).astype(jnp.float32)
             for first in range(0, width, 2 * slots)], axis=1).astype(jnp.bfloat16)
        total = jnp.dot(chosen, parts[kind, p, 0], preferred_element_type=jnp.float32)
        for piece in range(1, PIECES):
            total += jnp.dot(chosen, parts[kind, p, piece], preferred_element_type=jnp.float32)
        return total

    def skips(kind, p):
        return jnp.logical_and(gives, gives_cell == p) if kind == 0 else row < 0

    for t in tasks:
        @pl.when(jnp.logical_not(skips(*t[:2])))
        def _(t=t):
            handle(*t)

    def near_copy():
        s = core
        return pltpu.make_async_remote_copy(
            src_ref=near_out, dst_ref=rows_in.at[0, core, s], send_sem=near_sem.at[0], recv_sem=rows_recv.at[0, core, s],
            device_id=(row, even + 1 - core), device_id_type=MESH)

    @pl.when(holds)
    def _():
        push_copy.wait_recv()
        split_parts(held[...], parts, 2, 0)
        index_arrival(5 + core).wait_recv()
        near_out[...] = gathered(wanted[5 + core], core, 2, 0)
        near_copy().start()

        @pl.when(for_row != row)
        def _():
            index_arrival(6 - core).wait_recv()

        rows_in[0, core, 1 - core] = gathered(wanted[6 - core], core, 2, 0)

    for number in range(len(messages)):
        @pl.when(leaves(number))
        def _(number=number):
            index_copy(number).wait_send()

    for t in tasks[:cells * STEPS]:
        @pl.when(jnp.logical_not(jnp.logical_or(stays(*t), skips(*t[:2]))))
        def _(t=t):
            rows_copy(*t).wait_send()

    away = moved(row, col)
    for c in range(cells):
        total = None
        for s in range(STEPS):
            block = lax.rem(col + cells * for_row + c + s, n_col)
            close = jnp.logical_and(work_near[c], core == 1 - s)
            x_here = jnp.logical_and(jnp.logical_and(away == 0, block == col), jnp.logical_not(close))
            x_got = jnp.logical_or(x_here, jnp.logical_and(close, core == c))
            z_here = block // cells == row
            for kind, here in ((0, x_got), (1, z_here)):
                @pl.when(jnp.logical_not(here))
                def _(kind=kind, c=c, s=s):
                    pltpu.make_async_remote_copy(
                        src_ref=rows_out.at[kind, c, s], dst_ref=rows_in.at[kind, c, s], send_sem=rows_send.at[kind, c, s],
                        recv_sem=rows_recv.at[kind, c, s], device_id=(row, col), device_id_type=MESH).wait_recv()
            slot = lax.rem(block, cells)
            x_side = jnp.where(x_here, rows_out[0, c, s], rows_in[0, c, s])
            z_side = jnp.where(z_here, rows_out[1, slot, s], rows_in[1, c, s])
            term = x_side * z_side
            total = term if total is None else total + term
        folded = total[:, :slots]
        for at in range(slots, width, slots):
            folded = folded + total[:, at:at + slots]
        given[c] = jnp.sum(jnp.transpose(folded), axis=0, keepdims=True)

    given_copy = pltpu.make_async_remote_copy(
        src_ref=given, dst_ref=taken, send_sem=given_sem.at[0], recv_sem=given_sem.at[1],
        device_id=(twin, col), device_id_type=MESH)

    @pl.when(away == 1)
    def _():
        given_copy.start()

    for t in tasks[cells * STEPS:]:
        @pl.when(jnp.logical_not(jnp.logical_or(stays(*t), skips(*t[:2]))))
        def _(t=t):
            rows_copy(*t).wait_send()

    @pl.when(gives)
    def _():
        push_copy.wait_send()

    @pl.when(holds)
    def _():
        near_copy().wait_send()

    @pl.when(away == 1)
    def _():
        given_copy.wait()
        out_ref[...] = taken[...]

    @pl.when(away == 0)
    def _():
        out_ref[...] = given[...]


def body(x_iterate, z_inverse, edge_src, edge_dst, edge_count):
    height, width = x_iterate.shape
    cells, _, slots = edge_src.shape
    hbm = pl.BlockSpec(memory_space=pltpu.HBM)
    values = pl.pallas_call(
        kernel,
        out_shape=jax.ShapeDtypeStruct((cells, 1, slots), jnp.float32),
        in_specs=[hbm] * 4,
        out_specs=pl.BlockSpec(memory_space=pltpu.VMEM),
        scratch_shapes=[
            pltpu.VMEM((height, width), jnp.float32),
            pltpu.VMEM((height, width), jnp.float32),
            pltpu.VMEM((3, cells, PIECES, width, width), jnp.bfloat16),
            pltpu.VMEM((2, cells, 1, slots), jnp.int32),
            pltpu.VMEM((2, 1, cells * slots), jnp.int32),
            pltpu.VMEM((7, 1, cells * slots), jnp.int32),
            pltpu.VMEM((2, cells, STEPS, slots, width), jnp.float32),
            pltpu.VMEM((2, cells, STEPS, slots, width), jnp.float32),
            pltpu.VMEM((width, width), jnp.float32),
            pltpu.VMEM((slots, width), jnp.float32),
            pltpu.VMEM((cells, 1, slots), jnp.float32),
            pltpu.VMEM((cells, 1, slots), jnp.float32),
            pltpu.SemaphoreType.DMA((4,)),
            pltpu.SemaphoreType.DMA((6,)),
            pltpu.SemaphoreType.DMA((7,)),
            pltpu.SemaphoreType.DMA((2, cells, STEPS)),
            pltpu.SemaphoreType.DMA((2, cells, STEPS)),
            pltpu.SemaphoreType.DMA((2,)),
            pltpu.SemaphoreType.DMA((1,)),
            pltpu.SemaphoreType.DMA((2,)),
        ],
        compiler_params=pltpu.CompilerParams(collective_id=0, has_side_effects=True, vmem_limit_bytes=10 * 2**20),
        name="schur_row",
    )(*(pltpu.with_memory_space_constraint(operand, pltpu.HBM) for operand in (x_iterate, z_inverse, edge_src, edge_dst)))
    live = lax.broadcasted_iota(jnp.int32, values.shape, 2) < edge_count[:, :, None]
    return jnp.where(live, values, jnp.zeros_like(values))


def solution(mesh):
    return jax.shard_map(
        body,
        mesh=mesh,
        in_specs=(
            P("row", "col"),
            P("row", "col"),
            P("row", "col", None),
            P("row", "col", None),
            P("row", "col"),
        ),
        out_specs=P("row", "col", None),
        check_vma=False,
    )
```

```python
import jax
import jax.numpy as jnp
from jax import lax
from jax.experimental import pallas as pl
from jax.experimental.pallas import tpu as pltpu
from jax.sharding import PartitionSpec as P

STEPS = 2
PIECES = 2
MESH = pl.DeviceIdType.MESH


def split_parts(value, parts_ref, *index):
    rest = value
    for piece in range(PIECES):
        part = rest.astype(jnp.bfloat16)
        parts_ref[(*index, piece)] = part
        if piece + 1 < PIECES:
            rest = rest - part.astype(jnp.float32)


def kernel(
    x_hbm, z_hbm, src_hbm, dst_hbm, out_ref,
    x_vmem, z_vmem, parts, index_in, index_out, wanted, rows_out, rows_in, held, near_out, given, taken,
    local_sem, index_send, index_recv, rows_send, rows_recv, push_sem, near_sem, given_sem,
):
    row, col = lax.axis_index("row"), lax.axis_index("col")
    n_row, n_col = lax.axis_size("row"), lax.axis_size("col")
    slots = src_hbm.shape[2]
    width = parts.shape[3]
    cells = 2
    src_copy = pltpu.make_async_copy(src_hbm, index_in.at[0], local_sem.at[2])
    dst_copy = pltpu.make_async_copy(dst_hbm, index_in.at[1], local_sem.at[3])
    x_copy = pltpu.make_async_copy(x_hbm, x_vmem, local_sem.at[0])
    z_copy = pltpu.make_async_copy(z_hbm, z_vmem, local_sem.at[1])
    src_copy.start()
    dst_copy.start()
    x_copy.start()
    z_copy.start()

    layer, chips = n_row // 2, n_col // 4
    twin = lax.rem(row + layer, n_row)

    def moved(reader_row, reader_col):
        diagonal = lax.rem(reader_row, layer) + lax.rem(reader_col, n_col // 2) // 2
        return jnp.where(diagonal >= 6, 1 - reader_col // (n_col // 2), jnp.where(diagonal >= chips - 1, 0, reader_col // (n_col // 2)))

    def working(reader_row, reader_col):
        return lax.rem(reader_row + layer * moved(reader_row, reader_col), n_row)

    def pushed(reader_row, reader_col, q):
        x, y = lax.rem(reader_row, layer), lax.rem(reader_col, n_col // 2) // 2
        busy = jnp.logical_and((x + 1) // 2 == 1, reader_row != 1)
        return jnp.logical_and(jnp.logical_or(jnp.logical_and(x + y < chips, jnp.logical_or(reader_col < n_col // 2, busy)), jnp.logical_and(x + y < chips - 1, x == 0)), q == 1)

    core = lax.rem(col, 2)
    even = col - core
    for_row = working(row, col)
    gives_cell = 1 - core
    gives_to = lax.rem(col - cells * row - gives_cell - 1 + 2 * n_col, n_col)
    gives = pushed(row, gives_to, gives_cell)
    holds = pushed(for_row, even, core)
    giver = (for_row, lax.rem(even + cells * for_row + 1 + core, n_col))
    near = [pushed(row, even, c) for c in range(cells)]
    work_near = [pushed(for_row, even, c) for c in range(cells)]

    x_owner = [lax.rem(col + cells * row + u, n_col) for u in range(3)]
    x_reader = [lax.rem(col - cells * row - u + 2 * n_col, n_col) for u in range(3)]
    half = col // cells
    z_owner = [lax.rem(row + half + d, n_row) for d in range(2)]
    z_reader = [lax.rem(row - half - d + 2 * n_row, n_row) for d in range(2)]
    links = [((row, x_reader[u]), x_owner[u] == col) for u in range(3)]
    links += [((z_reader[d], col), z_owner[d] == row) for d in range(2)]
    barrier = pltpu.get_barrier_semaphore()
    for device in ((twin, col), (row, even + 1 - core), (twin, even + 1 - core)):
        pl.semaphore_signal(barrier, inc=1, device_id=device, device_id_type=MESH)

    @pl.when(holds)
    def _():
        pl.semaphore_signal(barrier, inc=1, device_id=giver, device_id_type=MESH)

    for reader, own in links:
        @pl.when(jnp.logical_not(own))
        def _():
            pl.semaphore_signal(barrier, inc=1, device_id=reader, device_id_type=MESH)

    src_copy.wait()
    dst_copy.wait()
    for which in range(2):
        index_out[which, :, :slots] = index_in[which, 0]
        index_out[which, :, slots:] = index_in[which, 1]
    pl.semaphore_wait(barrier, 3 + jnp.where(gives, 1, 0) + sum(jnp.where(own, 0, 1) for _, own in links))

    messages = [
        (0, (row, x_owner[u]), u, x_owner[u] == col, jnp.logical_and(near[1], core == 0) if u == 2 else None) for u in range(3)
    ]
    messages += [(1, (z_owner[d], col), 3 + d, z_owner[d] == row, None) for d in range(2)]
    messages += [(0, (for_row, even + 1), 6 - core, jnp.logical_and(for_row == row, core == 1), jnp.logical_not(near[1]))]

    def index_copy(number):
        which, device, slot, _, _ = messages[number]
        return pltpu.make_async_remote_copy(
            src_ref=index_out.at[which], dst_ref=wanted.at[slot], send_sem=index_send.at[number],
            recv_sem=index_recv.at[slot], device_id=device, device_id_type=MESH)

    def leaves(number):
        _, _, _, own, dropped = messages[number]
        out = jnp.logical_not(own)
        return out if dropped is None else jnp.logical_and(out, jnp.logical_not(dropped))

    for number in (0, 1, 2, 5, 3, 4):
        @pl.when(leaves(number))
        def _(number=number):
            index_copy(number).start()

        which, _, slot, own, dropped = messages[number]

        @pl.when(own if dropped is None else jnp.logical_and(own, jnp.logical_not(dropped)))
        def _(which=which, slot=slot):
            wanted[slot] = index_out[which]

    def index_arrival(slot):
        return pltpu.make_async_remote_copy(
            src_ref=index_out.at[0], dst_ref=wanted.at[slot], send_sem=index_send.at[0],
            recv_sem=index_recv.at[slot], device_id=(row, col), device_id_type=MESH)

    tasks = [(k, c, s) for k in (1, 0) for c in range(cells) for s in range(STEPS)]
    x_copy.wait()
    push_copy = pltpu.make_async_remote_copy(
        src_ref=x_vmem.at[pl.ds(pl.multiple_of(gives_cell * width, width), width)], dst_ref=held, send_sem=push_sem.at[0],
        recv_sem=push_sem.at[1], device_id=(working(row, gives_to), gives_to + gives_cell), device_id_type=MESH)

    @pl.when(gives)
    def _():
        push_copy.start()

    for c in range(cells):
        split_parts(x_vmem[c * width:(c + 1) * width, :], parts, 0, c)
    z_copy.wait()
    for b in range(cells):
        split_parts(jnp.transpose(z_vmem[b * width:(b + 1) * width, :]), parts, 1, b)

    def reader_of(kind, p, s):
        x_col = lax.rem(col - cells * row - p - s + 2 * n_col, n_col)
        block = lax.rem(cells * row + p - col - s + 2 * n_col, n_col)
        isz = kind == 1
        return jnp.where(isz, block // cells, row), jnp.where(isz, col, x_col), jnp.where(isz, lax.rem(block, cells), p)

    def rows_copy(kind, p, s):
        rrow, rcol, c = reader_of(kind, p, s)
        return pltpu.make_async_remote_copy(
            src_ref=rows_out.at[kind, p, s], dst_ref=rows_in.at[kind, c, s], send_sem=rows_send.at[kind, p, s],
            recv_sem=rows_recv.at[kind, c, s], device_id=(working(rrow, rcol), rcol), device_id_type=MESH)

    def stays(kind, p, s):
        rrow, rcol, c = reader_of(kind, p, s)
        return jnp.logical_and(working(rrow, rcol) == row, rcol == col)

    def handle(kind, p, s):
        rrow, rcol, c = reader_of(kind, p, s)
        slot = p + s if kind == 0 else 3 + (core + c + s) // 2
        arrives = jnp.logical_not(jnp.logical_and(rrow == row, rcol == col))
        if kind == 1 and p != s:
            arrives = jnp.logical_and(arrives, core == p)
        if (kind, p, s) != (0, 1, 0) and (kind, p, s) != (1, 1, 1):
            @pl.when(arrives)
            def _():
                index_arrival(slot).wait_recv()

        rows_out[kind, p, s] = gathered(wanted[slot], c, kind, p)

        @pl.when(jnp.logical_not(stays(kind, p, s)))
        def _():
            rows_copy(kind, p, s).start()

    def gathered(both, c, kind, p):
        upper = jnp.broadcast_to(c, both.shape) == 1
        mine = jnp.where(upper, pltpu.roll(both, slots, 1), both)
        down = jnp.transpose(jnp.broadcast_to(mine, (2 * slots, 2 * slots)))[:slots]
        chosen = jnp.concatenate(
            [(down == lax.broadcasted_iota(jnp.int32, down.shape, 1) + first).astype(jnp.float32)
             for first in range(0, width, 2 * slots)], axis=1).astype(jnp.bfloat16)
        total = jnp.dot(chosen, parts[kind, p, 0], preferred_element_type=jnp.float32)
        for piece in range(1, PIECES):
            total += jnp.dot(chosen, parts[kind, p, piece], preferred_element_type=jnp.float32)
        return total

    def skips(kind, p):
        return jnp.logical_and(gives, gives_cell == p) if kind == 0 else row < 0

    for t in tasks:
        @pl.when(jnp.logical_not(skips(*t[:2])))
        def _(t=t):
            handle(*t)

    def near_copy():
        s = core
        return pltpu.make_async_remote_copy(
            src_ref=near_out, dst_ref=rows_in.at[0, core, s], send_sem=near_sem.at[0], recv_sem=rows_recv.at[0, core, s],
            device_id=(row, even + 1 - core), device_id_type=MESH)

    @pl.when(holds)
    def _():
        push_copy.wait_recv()
        split_parts(held[...], parts, 2, 0)
        index_arrival(5 + core).wait_recv()
        near_out[...] = gathered(wanted[5 + core], core, 2, 0)
        near_copy().start()

        @pl.when(for_row != row)
        def _():
            index_arrival(6 - core).wait_recv()

        rows_in[0, core, 1 - core] = gathered(wanted[6 - core], core, 2, 0)

    for number in range(len(messages)):
        @pl.when(leaves(number))
        def _(number=number):
            index_copy(number).wait_send()

    for t in tasks[:cells * STEPS]:
        @pl.when(jnp.logical_not(jnp.logical_or(stays(*t), skips(*t[:2]))))
        def _(t=t):
            rows_copy(*t).wait_send()

    away = moved(row, col)
    for c in range(cells):
        total = None
        for s in range(STEPS):
            block = lax.rem(col + cells * for_row + c + s, n_col)
            close = jnp.logical_and(work_near[c], core == 1 - s)
            x_here = jnp.logical_and(jnp.logical_and(away == 0, block == col), jnp.logical_not(close))
            x_got = jnp.logical_or(x_here, jnp.logical_and(close, core == c))
            z_here = block // cells == row
            for kind, here in ((0, x_got), (1, z_here)):
                @pl.when(jnp.logical_not(here))
                def _(kind=kind, c=c, s=s):
                    pltpu.make_async_remote_copy(
                        src_ref=rows_out.at[kind, c, s], dst_ref=rows_in.at[kind, c, s], send_sem=rows_send.at[kind, c, s],
                        recv_sem=rows_recv.at[kind, c, s], device_id=(row, col), device_id_type=MESH).wait_recv()
            slot = lax.rem(block, cells)
            x_side = jnp.where(x_here, rows_out[0, c, s], rows_in[0, c, s])
            z_side = jnp.where(z_here, rows_out[1, slot, s], rows_in[1, c, s])
            term = x_side * z_side
            total = term if total is None else total + term
        folded = total[:, :slots]
        for at in range(slots, width, slots):
            folded = folded + total[:, at:at + slots]
        given[c] = jnp.sum(jnp.transpose(folded), axis=0, keepdims=True)

    given_copy = pltpu.make_async_remote_copy(
        src_ref=given, dst_ref=taken, send_sem=given_sem.at[0], recv_sem=given_sem.at[1],
        device_id=(twin, col), device_id_type=MESH)

    @pl.when(away == 1)
    def _():
        given_copy.start()

    for t in tasks[cells * STEPS:]:
        @pl.when(jnp.logical_not(jnp.logical_or(stays(*t), skips(*t[:2]))))
        def _(t=t):
            rows_copy(*t).wait_send()

    @pl.when(gives)
    def _():
        push_copy.wait_send()

    @pl.when(holds)
    def _():
        near_copy().wait_send()

    @pl.when(away == 1)
    def _():
        given_copy.wait()
        out_ref[...] = taken[...]

    @pl.when(away == 0)
    def _():
        out_ref[...] = given[...]


def body(x_iterate, z_inverse, edge_src, edge_dst, edge_count):
    height, width = x_iterate.shape
    cells, _, slots = edge_src.shape
    hbm = pl.BlockSpec(memory_space=pltpu.HBM)
    values = pl.pallas_call(
        kernel,
        out_shape=jax.ShapeDtypeStruct((cells, 1, slots), jnp.float32),
        in_specs=[hbm] * 4,
        out_specs=pl.BlockSpec(memory_space=pltpu.VMEM),
        scratch_shapes=[
            pltpu.VMEM((height, width), jnp.float32),
            pltpu.VMEM((height, width), jnp.float32),
            pltpu.VMEM((3, cells, PIECES, width, width), jnp.bfloat16),
            pltpu.VMEM((2, cells, 1, slots), jnp.int32),
            pltpu.VMEM((2, 1, cells * slots), jnp.int32),
            pltpu.VMEM((7, 1, cells * slots), jnp.int32),
            pltpu.VMEM((2, cells, STEPS, slots, width), jnp.float32),
            pltpu.VMEM((2, cells, STEPS, slots, width), jnp.float32),
            pltpu.VMEM((width, width), jnp.float32),
            pltpu.VMEM((slots, width), jnp.float32),
            pltpu.VMEM((cells, 1, slots), jnp.float32),
            pltpu.VMEM((cells, 1, slots), jnp.float32),
            pltpu.SemaphoreType.DMA((4,)),
            pltpu.SemaphoreType.DMA((6,)),
            pltpu.SemaphoreType.DMA((7,)),
            pltpu.SemaphoreType.DMA((2, cells, STEPS)),
            pltpu.SemaphoreType.DMA((2, cells, STEPS)),
            pltpu.SemaphoreType.DMA((2,)),
            pltpu.SemaphoreType.DMA((1,)),
            pltpu.SemaphoreType.DMA((2,)),
        ],
        compiler_params=pltpu.CompilerParams(collective_id=0, has_side_effects=True, vmem_limit_bytes=10 * 2**20),
        name="schur_row",
    )(*(pltpu.with_memory_space_constraint(operand, pltpu.HBM) for operand in (x_iterate, z_inverse, edge_src, edge_dst)))
    live = lax.broadcasted_iota(jnp.int32, values.shape, 2) < edge_count[:, :, None]
    return jnp.where(live, values, jnp.zeros_like(values))


def solution(mesh):
    return jax.shard_map(
        body,
        mesh=mesh,
        in_specs=(
            P("row", "col"),
            P("row", "col"),
            P("row", "col", None),
            P("row", "col", None),
            P("row", "col"),
        ),
        out_specs=P("row", "col", None),
        check_vma=False,
    )
```
